512 devices in a mesh: groups: 2 (over y), tp: 64 (over z, core), seq: 4 (over x).
Axes of the slice: x: 4, y: 2, z: 32, core: 2. Of those that a mesh axis runs over, the one named last changes fastest.
The devices are a block of a 4x8x32 slice.
Arguments:
- kv_prefill: bfloat16 [2, 2, 8, 32768, 128], P(None, None, 'groups', ('tp', 'seq')), parts along dimension 2, may hold values from -10 to 10
- queries: bfloat16 [2, 8, 64, 128], P(None, ('groups', 'seq'), 'tp'), parts along dimension 1, may hold values from -512 to 512
- new_kv: bfloat16 [2, 2, 8, 8, 128], P(None, None, ('groups', 'seq')), parts along dimension 2, may hold values from -4.5 to 4.5
- lengths: int32 [8], P(('groups', 'seq')), parts along dimension 0, may hold values from 2048 to 4095
- page_slots: int32 [8, 256], P(('groups', 'seq')), parts along dimension 0, may hold values from 0 to 255, each once within a row
Outputs:
- decode_pool: bfloat16 [2, 2, 64, 2048, 16, 128], P(None, None, 'tp', ('groups', 'seq')), parts along dimension 3
- attention_out: bfloat16 [2, 8, 64, 128], P(None, ('groups', 'seq'), 'tp'), parts along dimension 1
The draws below stay inside these ranges and needn't reach their ends.
There are 2 independent parts, one for each index of `groups`. The reference program is written for one: setup_inputs(seed, part) draws one part's arguments, and reference() takes and returns one part's arrays. A program takes and returns all parts, laid end to end along the dimension named above; each array names one. Nothing has to cross between parts.
Inputs may be any that keep to these rules, and one draw needn't show every extreme that they name: Row b belongs to sequence b: its page j goes to slot page_slots[b, j] of the row's block of 256 slots; each row uses every slot once.
All inputs are finite; a program needn't handle non-finite values.
Results may differ from the reference program's by a relative error of at most 0.01.
Values may be sent and summed in bfloat16 or wider, within the bound.
A program may use at most 64 MiB of HBM per device.

```python
import math
import jax
import jax.numpy as jnp
from jax import lax

LAYERS = 2
KVH = 8
QH = 64
DH = 128
PAGE = 16
CTX = 4096
SEQ_DEV = 1
SEQS = 4
PAGES = 256
COPIES = 64


def cache_and_query(key):
    cache_shape = (2, LAYERS, SEQS, KVH, CTX, DH)
    base_cache = jax.random.truncated_normal(jax.random.fold_in(key, 101), -4.5, 4.5, cache_shape, jnp.float32)
    base_query = jax.random.truncated_normal(jax.random.fold_in(key, 102), -4.5, 4.5, (LAYERS, SEQS, KVH, QH // KVH, DH), jnp.float32)
    cache_rows = base_cache
    query_rows = base_query
    return (cache_rows.reshape(2, LAYERS, SEQS, KVH * CTX, DH), query_rows.reshape(LAYERS, SEQS, QH, DH))


def draw_kv_prefill(key, part):
    return cache_and_query(key)[0].astype(jnp.bfloat16)


def draw_queries(key, part):
    return cache_and_query(key)[1].astype(jnp.bfloat16)


def with_ends(entries, stream_key, smallest, top_value):
    dims = entries.shape
    place = [jax.random.randint(jax.random.fold_in(stream_key, axis), (), 0, dims[axis]) for axis in range(len(dims))]
    entries = entries.at[tuple(place)].set(smallest)
    longest = dims.index(max(dims))
    place[longest] = (place[longest] + 1) % dims[longest]
    return entries.at[tuple(place)].set(top_value)


def block_scale(rng, shape, split, low, largest):
    factor_of = 1.0
    for axis_at, blocks in split:
        draws = jax.random.uniform(jax.random.fold_in(jax.random.fold_in(rng, 6), axis_at), (blocks,), jnp.float32, low / len(split), largest / len(split))
        factor_of = factor_of * jnp.repeat(jnp.exp(draws), shape[axis_at] // blocks).reshape((-1,) + (1,) * (len(shape) - 1 - axis_at))
    return factor_of


def gaussian(key, dims, scale, most, split=(), held_as=jnp.bfloat16):
    values = jax.random.normal(key, dims, jnp.float32) * scale
    if len(split) > 0:
        values = block_scale(key, dims, split, -0.22, 0.18) * values
    return jnp.clip(values, min=-most, max=most).astype(held_as)


def setup_inputs(seed: int = 0, part: int = 0) -> dict:
    seeds = jax.random.split(jax.random.key(seed), 6)
    own_keys = jax.random.split(jax.random.fold_in(seeds[5], part), 6)
    return {
        "kv_prefill": draw_kv_prefill(jax.random.fold_in(jax.random.fold_in(seeds[5], part), 71), part),
        "queries": draw_queries(jax.random.fold_in(jax.random.fold_in(seeds[5], part), 71), part),
        "new_kv": gaussian(own_keys[2], (2, LAYERS, SEQS, KVH, DH), 1.0, 4.5, ((2, 4),)),
        "lengths": with_ends(jax.random.randint(own_keys[3], (SEQS,), CTX // 2, CTX), jax.random.fold_in(own_keys[3], 1), CTX // 2, CTX - 1).astype(jnp.int32),
        "page_slots": jax.vmap(lambda own: jax.random.permutation(own, SEQ_DEV * PAGES))(jax.random.split(own_keys[4], (SEQS // SEQ_DEV))).reshape((SEQS // SEQ_DEV, SEQ_DEV * PAGES)).astype(jnp.int32),
    }


def reference(kv_prefill, queries, new_kv, lengths, page_slots):
    positions = jnp.arange(CTX, dtype=jnp.int32)
    arriving = positions[None, :] == lengths[:, None]
    cache_full = kv_prefill.reshape(2, LAYERS, SEQS, KVH, CTX, DH)
    cache_full = jnp.where(arriving[None, None, :, None, :, None], new_kv[:, :, :, :, None, :], cache_full)
    slots_block = SEQ_DEV * PAGES
    owners = jnp.arange(SEQS * PAGES, dtype=jnp.int32) // slots_block
    slot_index = owners * slots_block + page_slots.reshape(-1).astype(jnp.int32)
    paged_rows = cache_full.reshape(2, LAYERS, SEQS, KVH, PAGES, PAGE, DH).transpose(0, 1, 3, 2, 4, 5, 6)
    paged_rows = paged_rows.reshape(2, LAYERS, KVH, SEQS * PAGES, PAGE, DH)
    by_head = jnp.zeros_like(paged_rows).at[:, :, :, slot_index].set(paged_rows)
    copy_heads = jnp.arange(COPIES, dtype=jnp.int32) * KVH // COPIES
    decode_pool = jnp.take(by_head, copy_heads, axis=2)
    key_cache = cache_full[0].astype(jnp.float32)
    value_cache = cache_full[1].astype(jnp.float32)
    grouped_q = queries.astype(jnp.float32).reshape(LAYERS, SEQS, KVH, QH // KVH, DH)
    scores = jnp.einsum('lshgd,lshtd->lshgt', grouped_q, key_cache, precision=lax.Precision.HIGHEST) * (1.0 / math.sqrt(DH))
    visible = (positions[None, :] <= lengths[:, None])[None, :, None, None, :]
    masked = jnp.where(visible, scores, -1e+30)
    highest = lax.optimization_barrier(jnp.max(masked, axis=-1, keepdims=True))
    exponent = jnp.where(visible, jnp.exp(masked - highest), 0.0)
    weights = (exponent / lax.optimization_barrier(jnp.sum(exponent, axis=-1, keepdims=True))).astype(jnp.bfloat16)
    mixed_out = jnp.einsum('lshgt,lshtd->lshgd', weights.astype(jnp.float32), value_cache, precision=lax.Precision.HIGHEST)
    attention_out = mixed_out.astype(jnp.bfloat16).reshape(LAYERS, SEQS, QH, DH)
    return (decode_pool, attention_out)
```

```python
import functools
import math

import jax
import jax.numpy as jnp
from jax import lax
from jax.experimental import pallas as pl
from jax.experimental.pallas import tpu as pltpu
from jax.sharding import PartitionSpec as P

KVH = 8
PAGE = 16
CTX = 4096
CORES = 2
MESH = pl.DeviceIdType.MESH
MIB = 1 << 20


def arrival_order(chips, kinds):
    order = []
    for _ in range(chips - 1):
        further = [(hops + 1, kind) for hops, kind in order]
        own = [(1, kind) for kind in kinds]
        order = own[:-1] + further[:1] + own[-1:] + further[1:]
    return order


def spread_kernel(kv, cache, own_sem, pair_sem, x_sent, up_sent, down_sent, pair_sent):
    tp, x = lax.axis_index("tp"), lax.axis_index("seq")
    ranks, nx = lax.axis_size("tp"), lax.axis_size("seq")
    fan = ranks // KVH
    chips = fan // CORES
    rank = lax.rem(tp, fan)
    z, core = rank // CORES, lax.rem(tp, CORES)
    pages = kv.shape[3]
    last = chips - 1
    up, down, pair = {"tp": tp + CORES}, {"tp": tp - CORES}, {"tp": tp + 1 - 2 * core}

    def seq_rank(steps):
        return lax.rem(x + steps + nx, nx)

    barrier = pltpu.get_barrier_semaphore()

    def greet(device):
        pl.semaphore_signal(barrier, inc=1, device_id=device, device_id_type=MESH)

    greet(pair)
    for step in range(1, nx):
        greet({"seq": seq_rank(step)})
    pl.when(z < last)(lambda: greet(up))
    pl.when(z > 0)(lambda: greet(down))
    pl.semaphore_wait(barrier, nx + jnp.where(z < last, 1, 0) + jnp.where(z > 0, 1, 0))

    def place(plane, kind, of_core):
        first = ((plane * CORES + of_core) * nx + seq_rank(kind)) * pages
        return cache.at[:, :, pl.ds(first, pages)]

    def remote(src, dst, sent, landed, device):
        return pltpu.make_async_remote_copy(
            src_ref=src, dst_ref=dst, send_sem=sent, recv_sem=landed, device_id=device, device_id_type=MESH
        )

    def along(plane, kind, sent, device, src=None):
        index = plane * nx + kind
        block = place(plane, kind, core)
        return remote(block if src is None else src, block, sent.at[index], own_sem.at[index], device)

    def to_pair(plane, kind, src=None):
        index = plane * nx + kind
        block = place(plane, kind, core)
        return remote(block if src is None else src, block, pair_sent.at[index], pair_sem.at[index], pair)

    def to_seq(kind):
        mine = ((z * CORES + core) * nx + x) * pages
        target = seq_rank(-kind)
        return remote(
            kv.at[:, :, target],
            cache.at[:, :, pl.ds(mine, pages)],
            x_sent.at[kind],
            own_sem.at[z * nx + kind],
            {"seq": target},
        )

    kinds = [0, *sorted(range(1, nx), key=lambda k: (min(k, nx - k), k))]
    mine = kv.at[:, :, x]
    pl.when(z > 0)(lambda: along(z, 0, down_sent, down, mine).start())
    pl.when(z < last)(lambda: along(z, 0, up_sent, up, mine).start())
    for kind in kinds[1:]:
        to_seq(kind).start()
    local = pltpu.make_async_copy(mine, place(z, 0, core), own_sem.at[z * nx])
    local.start()
    to_pair(z, 0, mine).start()

    def landed(plane, kind):
        along(plane, kind, up_sent, up).wait_recv()

    def own(kind):
        landed(z, kind)
        pl.when(z > 0)(lambda: along(z, kind, down_sent, down).start())
        pl.when(z < last)(lambda: along(z, kind, up_sent, up).start())
        to_pair(z, kind).start()

    def from_above(hops, kind):
        landed(z + hops, kind)
        pl.when(z > 0)(lambda: along(z + hops, kind, down_sent, down).start())
        to_pair(z + hops, kind).start()

    def from_below(hops, kind):
        landed(z - hops, kind)
        pl.when(z < last)(lambda: along(z - hops, kind, up_sent, up).start())
        to_pair(z - hops, kind).start()

    def passing(hops, kind):
        pl.when(z + hops <= last)(lambda: from_above(hops, kind))
        pl.when(z - hops >= 0)(lambda: from_below(hops, kind))

    order = arrival_order(chips, kinds)
    for kind in kinds[1:-1]:
        own(kind)
    passing(*order[0])
    own(kinds[-1])
    for hops, kind in order[1:]:
        passing(hops, kind)

    local.wait()
    for kind in kinds[1:]:
        to_seq(kind).wait_send()
    for plane in range(chips):
        for kind in kinds:
            to_pair(plane, kind).wait_send()
            partner_block = place(plane, kind, 1 - core)
            index = plane * nx + kind
            remote(partner_block, partner_block, pair_sent.at[index], pair_sem.at[index], pair).wait_recv()

            def sent_down(plane=plane, kind=kind):
                along(plane, kind, down_sent, down).wait_send()

            def sent_up(plane=plane, kind=kind):
                along(plane, kind, up_sent, up).wait_send()

            pl.when(jnp.logical_and(z > 0, plane >= z))(sent_down)
            pl.when(jnp.logical_and(z < last, plane <= z))(sent_up)


def attend(length, q, k, v, k_new, v_new):
    scale = 1.0 / math.sqrt(q.shape[1])
    contract = (((1,), (1,)), ((), ()))
    q8 = jnp.broadcast_to(q, (8, q.shape[1]))
    scores = lax.dot_general(q8, k, contract, preferred_element_type=jnp.float32) * scale
    t = lax.broadcasted_iota(jnp.int32, scores.shape, 1)
    scores = jnp.where(t < length, scores, -1e30)
    fresh = jnp.sum(q8.astype(jnp.float32) * k_new.astype(jnp.float32), axis=1, keepdims=True) * scale
    top = jnp.maximum(jnp.max(scores, axis=1, keepdims=True), fresh)
    weights = jnp.where(t < length, jnp.exp(scores - top), 0.0)
    fresh = jnp.exp(fresh - top)
    total = jnp.sum(weights, axis=1, keepdims=True) + fresh
    weights = (weights / total).astype(jnp.bfloat16)
    fresh = (fresh / total).astype(jnp.bfloat16).astype(jnp.float32)
    mixed = jnp.dot(weights, v, preferred_element_type=jnp.float32)
    mixed = mixed + fresh * v_new.astype(jnp.float32)
    return mixed[:1].astype(jnp.bfloat16)


def page_kernel(lengths, slots, cache, queries, new_kv, pool, out, staged, sem):
    layers, pages, head = cache.shape[1], cache.shape[2], cache.shape[4]
    length = lengths[0]
    slot_now, row_now = slots[0, length // PAGE], lax.rem(length, PAGE)
    head_now = lax.axis_index("tp") * KVH // lax.axis_size("tp")
    rows = lax.broadcasted_iota(jnp.int32, (PAGE, head), 0)

    def fresh(kind, layer):
        block = new_kv[kind, layer, 0].astype(jnp.float32)
        mine = lax.broadcasted_iota(jnp.int32, block.shape, 0) == head_now
        return jnp.sum(jnp.where(mine, block, 0.0), axis=0, keepdims=True).astype(jnp.bfloat16)

    copies = []
    for kind in range(2):
        for layer in range(layers):

            def move(page, _, kind=kind, layer=layer):
                staged[kind, layer, slots[0, page]] = cache[kind, layer, page]
                return 0

            lax.fori_loop(0, pages, move, 0, unroll=16)
            tile = staged[kind, layer, slot_now].astype(jnp.float32)
            tile = jnp.where(rows == row_now, fresh(kind, layer).astype(jnp.float32), tile)
            staged[kind, layer, slot_now] = tile.astype(jnp.bfloat16)
            copy = pltpu.make_async_copy(
                staged.at[kind, layer], pool.at[kind, layer, 0], sem.at[kind * layers + layer]
            )
            copy.start()
            copies.append(copy)

    for layer in range(layers):
        out[layer : layer + 1] = attend(
            length,
            queries[layer : layer + 1],
            cache[0, layer].reshape(CTX, head),
            cache[1, layer].reshape(CTX, head),
            fresh(0, layer),
            fresh(1, layer),
        )
    for copy in copies:
        copy.wait()


def body(kv_prefill, queries, new_kv, lengths, page_slots):
    kinds, layers, seqs, positions, head = kv_prefill.shape
    nx = lax.axis_size("seq")
    fan = lax.axis_size("tp") // KVH
    count = fan // CORES * nx
    pages = CTX // PAGE
    dma = pltpu.SemaphoreType.DMA
    anywhere = pl.BlockSpec(memory_space=pl.ANY)
    vmem = pl.BlockSpec(memory_space=pltpu.VMEM)
    smem = pl.BlockSpec(memory_space=pltpu.SMEM)
    cache_shape = (kinds, layers, pages, PAGE, head)
    cache = pl.pallas_call(
        spread_kernel,
        out_shape=pltpu.VMEM(cache_shape, kv_prefill.dtype),
        in_specs=[pl.BlockSpec(memory_space=pltpu.HBM)],
        out_specs=vmem,
        scratch_shapes=[dma((count,)), dma((count,)), dma((nx,)), dma((count,)), dma((count,)), dma((count,))],
        compiler_params=pltpu.CompilerParams(collective_id=0, has_side_effects=True, vmem_limit_bytes=16 * MIB),
        name="spread",
    )(kv_prefill.reshape(kinds, layers, seqs, positions // PAGE, PAGE, head))
    pool, out = pl.pallas_call(
        page_kernel,
        out_shape=(
            jax.ShapeDtypeStruct((kinds, layers, 1, pages, PAGE, head), kv_prefill.dtype),
            jax.ShapeDtypeStruct((layers, head), queries.dtype),
        ),
        in_specs=[smem, smem, vmem, vmem, vmem],
        out_specs=(anywhere, vmem),
        scratch_shapes=[pltpu.VMEM(cache_shape, kv_prefill.dtype), dma((kinds * layers,))],
        compiler_params=pltpu.CompilerParams(vmem_limit_bytes=24 * MIB),
        name="pages",
    )(lengths, page_slots, cache, queries.reshape(layers, head), new_kv)
    return pool, out.reshape(queries.shape)


def solution(mesh):
    placed = (
        P(None, None, "groups", ("tp", "seq"), None),
        P(None, ("groups", "seq"), "tp", None),
        P(None, None, ("groups", "seq"), None, None),
        P(("groups", "seq")),
        P(("groups", "seq"), None),
    )
    return jax.shard_map(
        body,
        mesh=mesh,
        in_specs=placed,
        out_specs=(
            P(None, None, "tp", ("groups", "seq"), None, None),
            P(None, ("groups", "seq"), "tp", None),
        ),
        check_vma=False,
    )
```

```python
import functools
import math

import jax
import jax.numpy as jnp
from jax import lax
from jax.experimental import pallas as pl
from jax.experimental.pallas import tpu as pltpu
from jax.sharding import PartitionSpec as P

KVH = 8
PAGE = 16
CTX = 4096
CORES = 2
MESH = pl.DeviceIdType.MESH
MIB = 1 << 20


def arrival_order(chips, kinds):
    order = []
    for _ in range(chips - 1):
        further = [(hops + 1, kind) for hops, kind in order]
        own = [(1, kind) for kind in kinds]
        order = own[:-1] + further[:1] + own[-1:] + further[1:]
    return order


def spread_kernel(
    kv, cache, own_sem, pair_sem, x_sent, up_sent, down_sent, pair_sent, local_sem, up_here, first_here
):
    tp, x = lax.axis_index("tp"), lax.axis_index("seq")
    ranks, nx = lax.axis_size("tp"), lax.axis_size("seq")
    fan = ranks // KVH
    chips = fan // CORES
    rank = lax.rem(tp, fan)
    z, core = rank // CORES, lax.rem(tp, CORES)
    pages = kv.shape[3]
    last = chips - 1
    corner = jnp.logical_and(z == 0, x == 0)
    first = jnp.logical_and(corner, core == 0)
    stand_in = jnp.logical_and(corner, core == 1)
    usual = jnp.logical_not(corner)
    above_corner = jnp.logical_and(jnp.logical_and(z == 1, x == 0), core == 0)
    in_first_row = jnp.logical_and(jnp.logical_and(z == 0, core == 0), x > 0)
    pair = {"tp": tp + 1 - 2 * core}
    down = {"tp": tp - CORES + jnp.where(above_corner, 1, 0)}
    both = jnp.logical_and
    absent = jnp.logical_not(first)

    def seq_rank(steps):
        return lax.rem(x + steps + nx, nx)

    def up(of_core):
        return {"tp": tp + CORES + of_core - core}

    barrier = pltpu.get_barrier_semaphore()

    def signal(semaphore, device):
        pl.semaphore_signal(semaphore, inc=1, device_id=device, device_id_type=MESH)

    @pl.when(absent)
    def _():
        signal(barrier, pair)
        for step in range(1, nx):
            signal(barrier, {"seq": seq_rank(step)})
        pl.when(z < last)(lambda: signal(barrier, up(core)))
        pl.when(in_first_row)(lambda: signal(barrier, {"tp": tp + 1, "seq": 0}))
        pl.when(above_corner)(lambda: signal(barrier, {"tp": tp - CORES}))

    @pl.when(stand_in)
    def _():
        signal(barrier, up(0))
        for step in range(1, nx):
            signal(barrier, {"tp": tp - 1, "seq": step})

    greetings = jnp.where(first, nx + 1, jnp.where(stand_in, 2 * (nx - 1), nx + jnp.where(z > 0, 1, 0)))
    pl.semaphore_wait(barrier, greetings)
    pl.when(first)(lambda: signal(first_here, pair))
    pl.when(z > 0)(lambda: signal(up_here, down))

    def index(of_core, plane, kind):
        return (of_core * chips + plane) * nx + kind

    def place(of_core, plane, kind):
        start = ((plane * CORES + of_core) * nx + seq_rank(kind)) * pages
        return cache.at[:, :, pl.ds(start, pages)]

    def remote(src, dst, sent, landed, device):
        return pltpu.make_async_remote_copy(
            src_ref=src, dst_ref=dst, send_sem=sent, recv_sem=landed, device_id=device, device_id_type=MESH
        )

    def moved(sent, landed, device, of_core, plane, kind, src):
        at, block = index(of_core, plane, kind), place(of_core, plane, kind)
        return remote(block if src is None else src, block, sent.at[at], landed.at[at], device)

    def to_up(of_core, plane, kind, src=None):
        return moved(up_sent, own_sem, up(of_core), of_core, plane, kind, src)

    def to_down(plane, kind, src=None):
        return moved(down_sent, own_sem, down, core, plane, kind, src)

    def to_pair(of_core, plane, kind, src=None):
        return moved(pair_sent, pair_sem, pair, of_core, plane, kind, src)

    def to_seq(kind):
        target = seq_rank(-kind)
        aside = jnp.where(both(in_first_row, target == 0), 1, 0)
        start = ((z * CORES + core) * nx + x) * pages
        return remote(
            kv.at[:, :, target],
            cache.at[:, :, pl.ds(start, pages)],
            x_sent.at[kind],
            own_sem.at[index(core, z, kind)],
            {"tp": tp + aside, "seq": target},
        )

    kinds = [0, *sorted(range(1, nx), key=lambda k: (min(k, nx - k), k))]
    mine = kv.at[:, :, x]
    pl.when(first)(lambda: to_up(0, 0, 0, mine).start())
    pl.when(z > 0)(lambda: to_down(z, 0, mine).start())
    for kind in kinds[1:]:
        to_seq(kind).start()
    pl.when(jnp.logical_not(stand_in))(lambda: to_pair(core, z, 0, mine).start())
    local = pltpu.make_async_copy(mine, place(core, z, 0), local_sem)
    local.start()

    @pl.when(both(absent, z < last))
    def _():
        pl.semaphore_wait(up_here, jnp.where(stand_in, 2, 1))
        to_up(core, z, 0, mine).start()

    def arrive(of_core, plane, kind):
        to_up(of_core, plane, kind).wait_recv()

    def from_first(of_core, plane, kind):
        return both(jnp.logical_and(plane == 0, of_core == 0), seq_rank(kind) == 0)

    def own(kind):
        @pl.when(both(absent, jnp.logical_not(from_first(core, z, kind))))
        def _():
            arrive(core, z, kind)
            pl.when(z > 0)(lambda: to_down(z, kind).start())
            pl.when(z < last)(lambda: to_up(core, z, kind).start())
            pl.when(usual)(lambda: to_pair(core, z, kind).start())

        @pl.when(stand_in)
        def _():
            arrive(0, z, kind)
            to_up(0, z, kind).start()

    def passing(hops, kind, first_is_here):
        @pl.when(both(absent, z + hops <= last))
        def _():
            arrive(core, z + hops, kind)
            pl.when(z > 0)(lambda: to_down(z + hops, kind).start())
            pl.when(usual)(lambda: to_pair(core, z + hops, kind).start())

            @pl.when(stand_in)
            def _():
                arrive(0, hops, kind)
                if first_is_here:
                    to_pair(0, hops, kind).start()
                    to_pair(1, hops, kind).start()

        @pl.when(both(z - hops >= 0, jnp.logical_not(from_first(core, z - hops, kind))))
        def _():
            arrive(core, z - hops, kind)
            pl.when(z < last)(lambda: to_up(core, z - hops, kind).start())
            to_pair(core, z - hops, kind).start()

    def pass_first():
        kind = lax.rem(nx - x, nx)
        arrive(0, 0, kind)
        pl.when(z < last)(lambda: to_up(0, 0, kind).start())
        to_pair(0, 0, kind).start()

    order = arrival_order(chips, kinds)
    early = 2 * len(order) // 3
    for kind in kinds[1:-1]:
        own(kind)
    passing(*order[0], False)
    own(kinds[-1])
    for hops, kind in order[1:early]:
        passing(hops, kind, False)
    pl.when(in_first_row)(pass_first)

    @pl.when(stand_in)
    def _():
        pl.semaphore_wait(first_here, 1)
        to_pair(1, 0, 0, mine).start()
        for kind in kinds[1:]:
            to_pair(0, 0, kind).start()
            to_pair(1, 0, kind).start()
        for hops, kind in order[:early]:
            to_pair(0, hops, kind).start()
            to_pair(1, hops, kind).start()

    for hops, kind in order[early:]:
        passing(hops, kind, True)
    pl.when(both(z > 0, core == 0))(pass_first)

    local.wait()
    for kind in kinds[1:]:
        to_seq(kind).wait_send()
    pl.when(first)(lambda: to_up(0, 0, 0).wait_send())
    for plane in range(chips):
        for kind in kinds:

            @pl.when(usual)
            def _(plane=plane, kind=kind):
                to_pair(core, plane, kind).wait_send()
                to_pair(1 - core, plane, kind).wait_recv()

            for of_core in range(CORES):
                if (of_core, plane, kind) != (0, 0, 0):
                    pl.when(stand_in)(lambda a=(of_core, plane, kind): to_pair(*a).wait_send())
                    pl.when(first)(lambda a=(of_core, plane, kind): to_pair(*a).wait_recv())

            pl.when(both(z > 0, plane >= z))(lambda a=(plane, kind): to_down(*a).wait_send())
            pl.when(both(both(absent, z < last), plane <= z))(lambda a=(plane, kind): to_up(core, *a).wait_send())
    pl.when(first)(lambda: to_pair(0, 0, 0).wait_send())

    @pl.when(stand_in)
    def _():
        to_pair(0, 0, 0).wait_recv()
        for kind in kinds[1:]:
            to_up(0, 0, kind).wait_send()


def attend(length, q, k, v, k_new, v_new):
    scale = 1.0 / math.sqrt(q.shape[1])
    contract = (((1,), (1,)), ((), ()))
    q8 = jnp.broadcast_to(q, (8, q.shape[1]))
    scores = lax.dot_general(q8, k, contract, preferred_element_type=jnp.float32) * scale
    t = lax.broadcasted_iota(jnp.int32, scores.shape, 1)
    scores = jnp.where(t < length, scores, -1e30)
    fresh = jnp.sum(q8.astype(jnp.float32) * k_new.astype(jnp.float32), axis=1, keepdims=True) * scale
    top = jnp.maximum(jnp.max(scores, axis=1, keepdims=True), fresh)
    weights = jnp.where(t < length, jnp.exp(scores - top), 0.0)
    fresh = jnp.exp(fresh - top)
    total = jnp.sum(weights, axis=1, keepdims=True) + fresh
    weights = (weights / total).astype(jnp.bfloat16)
    fresh = (fresh / total).astype(jnp.bfloat16).astype(jnp.float32)
    mixed = jnp.dot(weights, v, preferred_element_type=jnp.float32)
    mixed = mixed + fresh * v_new.astype(jnp.float32)
    return mixed[:1].astype(jnp.bfloat16)


def page_kernel(lengths, slots, cache, queries, new_kv, pool, out, staged, sem):
    layers, pages, head = cache.shape[1], cache.shape[2], cache.shape[4]
    length = lengths[0]
    slot_now, row_now = slots[0, length // PAGE], lax.rem(length, PAGE)
    head_now = lax.axis_index("tp") * KVH // lax.axis_size("tp")
    rows = lax.broadcasted_iota(jnp.int32, (PAGE, head), 0)

    def fresh(kind, layer):
        block = new_kv[kind, layer, 0].astype(jnp.float32)
        mine = lax.broadcasted_iota(jnp.int32, block.shape, 0) == head_now
        return jnp.sum(jnp.where(mine, block, 0.0), axis=0, keepdims=True).astype(jnp.bfloat16)

    copies = []
    for kind in range(2):
        for layer in range(layers):

            def move(page, _, kind=kind, layer=layer):
                staged[kind, layer, slots[0, page]] = cache[kind, layer, page]
                return 0

            lax.fori_loop(0, pages, move, 0, unroll=16)
            tile = staged[kind, layer, slot_now].astype(jnp.float32)
            tile = jnp.where(rows == row_now, fresh(kind, layer).astype(jnp.float32), tile)
            staged[kind, layer, slot_now] = tile.astype(jnp.bfloat16)
            copy = pltpu.make_async_copy(
                staged.at[kind, layer], pool.at[kind, layer, 0], sem.at[kind * layers + layer]
            )
            copy.start()
            copies.append(copy)

    for layer in range(layers):
        out[layer : layer + 1] = attend(
            length,
            queries[layer : layer + 1],
            cache[0, layer].reshape(CTX, head),
            cache[1, layer].reshape(CTX, head),
            fresh(0, layer),
            fresh(1, layer),
        )
    for copy in copies:
        copy.wait()


def body(kv_prefill, queries, new_kv, lengths, page_slots):
    kinds, layers, seqs, positions, head = kv_prefill.shape
    nx = lax.axis_size("seq")
    fan = lax.axis_size("tp") // KVH
    count = fan * nx
    pages = CTX // PAGE
    dma = pltpu.SemaphoreType.DMA
    anywhere = pl.BlockSpec(memory_space=pl.ANY)
    vmem = pl.BlockSpec(memory_space=pltpu.VMEM)
    smem = pl.BlockSpec(memory_space=pltpu.SMEM)
    cache_shape = (kinds, layers, pages, PAGE, head)
    cache = pl.pallas_call(
        spread_kernel,
        out_shape=pltpu.VMEM(cache_shape, kv_prefill.dtype),
        in_specs=[pl.BlockSpec(memory_space=pltpu.HBM)],
        out_specs=vmem,
        scratch_shapes=[
            dma((count,)),
            dma((count,)),
            dma((nx,)),
            dma((count,)),
            dma((count,)),
            dma((count,)),
            dma,
            pltpu.SemaphoreType.REGULAR,
            pltpu.SemaphoreType.REGULAR,
        ],
        compiler_params=pltpu.CompilerParams(collective_id=0, has_side_effects=True, vmem_limit_bytes=16 * MIB),
        name="spread",
    )(kv_prefill.reshape(kinds, layers, seqs, positions // PAGE, PAGE, head))
    pool, out = pl.pallas_call(
        page_kernel,
        out_shape=(
            jax.ShapeDtypeStruct((kinds, layers, 1, pages, PAGE, head), kv_prefill.dtype),
            jax.ShapeDtypeStruct((layers, head), queries.dtype),
        ),
        in_specs=[smem, smem, vmem, vmem, vmem],
        out_specs=(anywhere, vmem),
        scratch_shapes=[pltpu.VMEM(cache_shape, kv_prefill.dtype), dma((kinds * layers,))],
        compiler_params=pltpu.CompilerParams(vmem_limit_bytes=24 * MIB),
        name="pages",
    )(lengths, page_slots, cache, queries.reshape(layers, head), new_kv)
    return pool, out.reshape(queries.shape)


def solution(mesh):
    placed = (
        P(None, None, "groups", ("tp", "seq"), None),
        P(None, ("groups", "seq"), "tp", None),
        P(None, None, ("groups", "seq"), None, None),
        P(("groups", "seq")),
        P(("groups", "seq"), None),
    )
    return jax.shard_map(
        body,
        mesh=mesh,
        in_specs=placed,
        out_specs=(
            P(None, None, "tp", ("groups", "seq"), None, None),
            P(None, ("groups", "seq"), "tp", None),
        ),
        check_vma=False,
    )
```

```python
import functools
import math

import jax
import jax.numpy as jnp
from jax import lax
from jax.experimental import pallas as pl
from jax.experimental.pallas import tpu as pltpu
from jax.sharding import PartitionSpec as P

KVH = 8
PAGE = 16
CTX = 4096
CORES = 2
MESH = pl.DeviceIdType.MESH
MIB = 1 << 20
GROUP = 8


def arrival_order(chips, kinds):
    order = []
    for _ in range(chips - 1):
        further = [(hops + 1, kind) for hops, kind in order]
        own = [(1, kind) for kind in kinds]
        order = own[:-1] + further[:1] + own[-1:] + further[1:]
    return order


def spread_kernel(
    kv,
    cache,
    own_sem,
    pair_sem,
    first_sem,
    first_pair_sem,
    x_sent,
    up_sent,
    down_sent,
    pair_sent,
    first_sent,
    first_up_sent,
    first_pair_sent,
    local_sem,
    up_here,
    first_here,
):
    tp, x = lax.axis_index("tp"), lax.axis_index("seq")
    ranks, nx = lax.axis_size("tp"), lax.axis_size("seq")
    fan = ranks // KVH
    chips = fan // CORES
    rank = lax.rem(tp, fan)
    z, core = rank // CORES, lax.rem(tp, CORES)
    layers, pages = kv.shape[1], kv.shape[3]
    pieces = [(kind, layer) for kind in range(kv.shape[0]) for layer in range(layers)]
    last = chips - 1
    both, no = jnp.logical_and, jnp.logical_not
    corner = both(z == 0, x == 0)
    first = both(corner, core == 0)
    stand_in = both(corner, core == 1)
    usual, absent = no(corner), no(first)
    above = both(z == 1, x == 0)
    row = both(z == 0, x > 0)
    pair = {"tp": tp + 1 - 2 * core}
    down = {"tp": tp - CORES + jnp.where(both(above, core == 0), 1, 0)}

    def seq_rank(steps):
        return lax.rem(x + steps + nx, nx)

    def up(of_core):
        return {"tp": tp + CORES + of_core - core}

    def along_seq(steps):
        target = seq_rank(steps)
        aside = jnp.where(both(both(row, core == 0), target == 0), 1, 0)
        return {"tp": tp + aside, "seq": target}

    barrier = pltpu.get_barrier_semaphore()

    def signal(semaphore, device):
        pl.semaphore_signal(semaphore, inc=1, device_id=device, device_id_type=MESH)

    @pl.when(absent)
    def _():
        signal(barrier, pair)
        for step in range(1, nx):
            signal(barrier, along_seq(step))
        pl.when(z < last)(lambda: signal(barrier, up(core)))
        pl.when(both(row, core == 1))(lambda: signal(barrier, {"tp": tp - 1, "seq": 0}))
        pl.when(both(above, core == 1))(lambda: signal(barrier, {"tp": tp - CORES - 1}))

    @pl.when(stand_in)
    def _():
        signal(barrier, up(0))
        for step in range(1, nx):
            signal(barrier, {"tp": tp - 1, "seq": step})

    greetings = jnp.where(first, nx + 1, jnp.where(stand_in, 2 * (nx - 1), nx + jnp.where(z > 0, 1, 0)))
    pl.semaphore_wait(barrier, greetings)
    pl.when(z > 0)(lambda: signal(up_here, down))

    def index(of_core, plane, kind):
        return (of_core * chips + plane) * nx + kind

    def start_of(of_core, plane, kind):
        return ((plane * CORES + of_core) * nx + seq_rank(kind)) * pages

    def place(of_core, plane, kind):
        return cache.at[:, :, pl.ds(start_of(of_core, plane, kind), pages)]

    def remote(src, dst, sent, landed, device):
        return pltpu.make_async_remote_copy(
            src_ref=src, dst_ref=dst, send_sem=sent, recv_sem=landed, device_id=device, device_id_type=MESH
        )

    def moved(sent, landed, device, of_core, plane, kind, src):
        at, block = index(of_core, plane, kind), place(of_core, plane, kind)
        return remote(block if src is None else src, block, sent.at[at], landed.at[at], device)

    def to_up(of_core, plane, kind, src=None):
        return moved(up_sent, own_sem, up(of_core), of_core, plane, kind, src)

    def to_down(plane, kind, src=None):
        return moved(down_sent, own_sem, down, core, plane, kind, src)

    def to_pair(of_core, plane, kind, src=None):
        return moved(pair_sent, pair_sem, pair, of_core, plane, kind, src)

    def to_seq(kind):
        start = ((z * CORES + core) * nx + x) * pages
        return remote(
            kv.at[:, :, seq_rank(-kind)],
            cache.at[:, :, pl.ds(start, pages)],
            x_sent.at[kind],
            own_sem.at[index(core, z, kind)],
            along_seq(-kind),
        )

    def first_piece(piece):
        kind, layer = pieces[piece]
        start = start_of(0, 0, lax.rem(nx - x, nx))
        return cache.at[kind, layer, pl.ds(start, pages)]

    def first_to(steps, piece, device, sent):
        kind, layer = pieces[piece]
        return remote(
            kv.at[kind, layer, steps],
            cache.at[kind, layer, pl.ds(0, pages)],
            first_sent.at[sent * len(pieces) + piece],
            first_sem.at[piece],
            device,
        )

    def first_targets(piece):
        away = [first_to(k, piece, {"tp": tp + 1, "seq": k}, k) for k in first_order]
        here = [first_to(0, piece, pair, 0), first_to(0, piece, {"tp": tp + CORES + 1}, nx)]
        return away, here

    def first_up(piece):
        block = first_piece(piece)
        return remote(block, block, first_up_sent.at[piece], first_sem.at[piece], up(core))

    def first_pair(piece):
        block = first_piece(piece)
        return remote(block, block, first_pair_sent.at[piece], first_pair_sem.at[piece], pair)

    kinds = [0, *sorted(range(1, nx), key=lambda k: (min(k, nx - k), k))]
    first_order = kinds[1:]
    mine = kv.at[:, :, x]

    @pl.when(first)
    def _():
        signal(first_here, pair)
        sends = [first_targets(piece) for piece in range(len(pieces))]
        for _, here in sends:
            here[1].start()
        for place_in_order in range(nx - 1):
            for away, _ in sends:
                away[place_in_order].start()
        for _, here in sends:
            here[0].start()

    pl.when(z > 0)(lambda: to_down(z, 0, mine).start())

    @pl.when(absent)
    def _():
        for kind in kinds[1:]:
            to_seq(kind).start()

    pl.when(usual)(lambda: to_pair(core, z, 0, mine).start())
    local = pltpu.make_async_copy(mine, place(core, z, 0), local_sem)
    local.start()

    @pl.when(both(absent, z < last))
    def _():
        pl.semaphore_wait(up_here, jnp.where(stand_in, 2, 1))
        to_up(core, z, 0, mine).start()

    def arrive(of_core, plane, kind):
        to_up(of_core, plane, kind).wait_recv()

    def from_first(of_core, plane, kind):
        return both(both(plane == 0, of_core == 0), seq_rank(kind) == 0)

    def own(kind):
        @pl.when(both(absent, no(from_first(core, z, kind))))
        def _():
            arrive(core, z, kind)
            pl.when(z > 0)(lambda: to_down(z, kind).start())
            pl.when(z < last)(lambda: to_up(core, z, kind).start())
            pl.when(usual)(lambda: to_pair(core, z, kind).start())

        @pl.when(stand_in)
        def _():
            arrive(0, z, kind)
            to_up(0, z, kind).start()

    def passing(hops, kind, first_is_here):
        @pl.when(both(absent, z + hops <= last))
        def _():
            arrive(core, z + hops, kind)
            pl.when(z > 0)(lambda: to_down(z + hops, kind).start())
            pl.when(usual)(lambda: to_pair(core, z + hops, kind).start())

            @pl.when(stand_in)
            def _():
                arrive(0, hops, kind)
                if first_is_here:
                    to_pair(0, hops, kind).start()
                    to_pair(1, hops, kind).start()

        @pl.when(both(z - hops >= 0, no(from_first(core, z - hops, kind))))
        def _():
            arrive(core, z - hops, kind)
            pl.when(z < last)(lambda: to_up(core, z - hops, kind).start())
            to_pair(core, z - hops, kind).start()

    def pass_first():
        for piece in range(len(pieces)):
            first_up(piece).wait_recv()
            pl.when(both(z < last, usual))(lambda: first_up(piece).start())
            pl.when(usual)(lambda: first_pair(piece).start())

    order = arrival_order(chips, kinds)
    early = 2 * len(order) // 3
    for kind in kinds[1:-1]:
        own(kind)
    passing(*order[0], False)
    own(kinds[-1])
    for hops, kind in order[1:early]:
        passing(hops, kind, False)
    pl.when(both(row, core == 1))(pass_first)

    @pl.when(stand_in)
    def _():
        pl.semaphore_wait(first_here, 1)
        to_pair(1, 0, 0, mine).start()
        for kind in kinds[1:]:
            to_pair(0, 0, kind).start()
            to_pair(1, 0, kind).start()
        for hops, kind in order[:early]:
            to_pair(0, hops, kind).start()
            to_pair(1, hops, kind).start()

    for hops, kind in order[early:]:
        passing(hops, kind, True)
    pl.when(both(jnp.logical_or(z > 0, stand_in), core == 1))(pass_first)

    local.wait()

    @pl.when(absent)
    def _():
        for kind in kinds[1:]:
            to_seq(kind).wait_send()

    for plane in range(chips):
        for kind in kinds:

            @pl.when(both(usual, no(from_first(core, plane, kind))))
            def _(plane=plane, kind=kind):
                to_pair(core, plane, kind).wait_send()

            @pl.when(both(usual, no(from_first(1 - core, plane, kind))))
            def _(plane=plane, kind=kind):
                to_pair(1 - core, plane, kind).wait_recv()

            for of_core in range(CORES):
                if (of_core, plane, kind) != (0, 0, 0):
                    pl.when(stand_in)(lambda a=(of_core, plane, kind): to_pair(*a).wait_send())
                    pl.when(first)(lambda a=(of_core, plane, kind): to_pair(*a).wait_recv())

            pl.when(both(z > 0, plane >= z))(lambda a=(plane, kind): to_down(*a).wait_send())

            @pl.when(both(both(absent, z < last), both(plane <= z, no(from_first(core, plane, kind)))))
            def _(plane=plane, kind=kind):
                to_up(core, plane, kind).wait_send()

    for piece in range(len(pieces)):

        @pl.when(both(usual, core == 1))
        def _(piece=piece):
            pl.when(z < last)(lambda: first_up(piece).wait_send())
            first_pair(piece).wait_send()

        pl.when(both(usual, core == 0))(lambda: first_pair(piece).wait_recv())

        @pl.when(first)
        def _(piece=piece):
            away, here = first_targets(piece)
            for copy in away + here:
                copy.wait_send()

    @pl.when(stand_in)
    def _():
        for kind in kinds[1:]:
            to_up(0, 0, kind).wait_send()


def attend(length, q, k, v, k_new, v_new):
    scale = 1.0 / math.sqrt(q.shape[1])
    contract = (((1,), (1,)), ((), ()))
    q8 = jnp.broadcast_to(q, (8, q.shape[1]))
    scores = lax.dot_general(q8, k, contract, preferred_element_type=jnp.float32) * scale
    t = lax.broadcasted_iota(jnp.int32, scores.shape, 1)
    scores = jnp.where(t < length, scores, -1e30)
    fresh = jnp.sum(q8.astype(jnp.float32) * k_new.astype(jnp.float32), axis=1, keepdims=True) * scale
    top = jnp.maximum(jnp.max(scores, axis=1, keepdims=True), fresh)
    weights = jnp.where(t < length, jnp.exp(scores - top), 0.0)
    fresh = jnp.exp(fresh - top)
    total = jnp.sum(weights, axis=1, keepdims=True) + fresh
    weights = (weights / total).astype(jnp.bfloat16)
    fresh = (fresh / total).astype(jnp.bfloat16).astype(jnp.float32)
    mixed = jnp.dot(weights, v, preferred_element_type=jnp.float32)
    mixed = mixed + fresh * v_new.astype(jnp.float32)
    return mixed[:1].astype(jnp.bfloat16)


def page_kernel(lengths, slots, cache, queries, new_kv, pool, out, tile, sem, tile_sem):
    kinds, layers, pages, head = cache.shape[0], cache.shape[1], cache.shape[2], cache.shape[4]
    length = lengths[0]
    page_now, row_now = length // PAGE, lax.rem(length, PAGE)
    head_now = lax.axis_index("tp") * KVH // lax.axis_size("tp")
    rows = lax.broadcasted_iota(jnp.int32, (PAGE, head), 0)

    def fresh(kind, layer):
        block = new_kv[kind, layer, 0].astype(jnp.float32)
        mine = lax.broadcasted_iota(jnp.int32, block.shape, 0) == head_now
        return jnp.sum(jnp.where(mine, block, 0.0), axis=0, keepdims=True)

    for kind in range(kinds):
        for layer in range(layers):
            held = cache[kind, layer, page_now].astype(jnp.float32)
            tile[kind, layer] = jnp.where(rows == row_now, fresh(kind, layer), held).astype(tile.dtype)

    def place(page):
        return pool.at[:, :, 0, slots[0, page]]

    def put(page):
        pltpu.make_async_copy(cache.at[:, :, page], place(page), sem).start()

    def put_group(group, _):
        @pl.when(group != page_now // GROUP)
        def _():
            for page in range(GROUP):
                put(group * GROUP + page)

        return 0

    lax.fori_loop(0, pages // GROUP, put_group, 0)
    for step in range(1, GROUP):
        put(page_now // GROUP * GROUP + lax.rem(page_now + step, GROUP))
    placed = pltpu.make_async_copy(tile, place(page_now), tile_sem)
    placed.start()

    for layer in range(layers):
        out[layer : layer + 1] = attend(
            length,
            queries[layer : layer + 1],
            cache[0, layer].reshape(CTX, head),
            cache[1, layer].reshape(CTX, head),
            fresh(0, layer).astype(queries.dtype),
            fresh(1, layer).astype(queries.dtype),
        )
    others = cache.at[:, :, pl.ds(1, pages - 1)]
    pltpu.make_async_copy(others, pool.at[:, :, 0, pl.ds(1, pages - 1)], sem).wait()
    placed.wait()


def body(kv_prefill, queries, new_kv, lengths, page_slots):
    kinds, layers, seqs, positions, head = kv_prefill.shape
    nx = lax.axis_size("seq")
    fan = lax.axis_size("tp") // KVH
    count = fan * nx
    pages = CTX // PAGE
    pieces = kinds * layers
    dma = pltpu.SemaphoreType.DMA
    anywhere = pl.BlockSpec(memory_space=pl.ANY)
    vmem = pl.BlockSpec(memory_space=pltpu.VMEM)
    smem = pl.BlockSpec(memory_space=pltpu.SMEM)
    cache_shape = (kinds, layers, pages, PAGE, head)
    blocks = kv_prefill.reshape(kinds, layers, seqs, positions // PAGE, PAGE, head)
    cache = pl.pallas_call(
        spread_kernel,
        out_shape=pltpu.VMEM(cache_shape, kv_prefill.dtype),
        in_specs=[pl.BlockSpec(memory_space=pltpu.HBM)],
        out_specs=vmem,
        scratch_shapes=[
            dma((count,)),
            dma((count,)),
            dma((pieces,)),
            dma((pieces,)),
            dma((nx,)),
            dma((count,)),
            dma((count,)),
            dma((count,)),
            dma(((nx + 1) * pieces,)),
            dma((pieces,)),
            dma((pieces,)),
            dma,
            pltpu.SemaphoreType.REGULAR,
            pltpu.SemaphoreType.REGULAR,
        ],
        compiler_params=pltpu.CompilerParams(collective_id=0, has_side_effects=True, vmem_limit_bytes=16 * MIB),
        name="spread",
    )(pltpu.with_memory_space_constraint(blocks, pltpu.HBM))
    pool, out = pl.pallas_call(
        page_kernel,
        out_shape=(
            jax.ShapeDtypeStruct((kinds, layers, 1, pages, PAGE, head), kv_prefill.dtype),
            jax.ShapeDtypeStruct((layers, head), queries.dtype),
        ),
        in_specs=[smem, smem, vmem, vmem, vmem],
        out_specs=(anywhere, vmem),
        scratch_shapes=[pltpu.VMEM((kinds, layers, PAGE, head), kv_prefill.dtype), dma, dma],
        compiler_params=pltpu.CompilerParams(vmem_limit_bytes=24 * MIB),
        name="pages",
    )(lengths, page_slots, cache, queries.reshape(layers, head), new_kv)
    return pool, out.reshape(queries.shape)


def solution(mesh):
    placed = (
        P(None, None, "groups", ("tp", "seq"), None),
        P(None, ("groups", "seq"), "tp", None),
        P(None, None, ("groups", "seq"), None, None),
        P(("groups", "seq")),
        P(("groups", "seq"), None),
    )
    return jax.shard_map(
        body,
        mesh=mesh,
        in_specs=placed,
        out_specs=(
            P(None, None, "tp", ("groups", "seq"), None, None),
            P(None, ("groups", "seq"), "tp", None),
        ),
        check_vma=False,
    )
```

```python
import functools
import math

import jax
import jax.numpy as jnp
from jax import lax
from jax.experimental import pallas as pl
from jax.experimental.pallas import tpu as pltpu
from jax.sharding import PartitionSpec as P

KVH = 8
PAGE = 16
CTX = 4096
CORES = 2
MESH = pl.DeviceIdType.MESH
MIB = 1 << 20


def arrival_order(chips, kinds):
    order = []
    for _ in range(chips - 1):
        further = [(hops + 1, kind) for hops, kind in order]
        own = [(1, kind) for kind in kinds]
        order = own[:-1] + further[:1] + own[-1:] + further[1:]
    return order


def spread_kernel(
    kv,
    slots,
    queries,
    new_kv,
    cache,
    slots_here,
    queries_here,
    new_kv_here,
    own_sem,
    pair_sem,
    first_sem,
    first_pair_sem,
    bulk_sem,
    x_sent,
    up_sent,
    down_sent,
    pair_sent,
    first_sent,
    first_up_sent,
    first_pair_sent,
    bulk_sent,
    local_sem,
    small_sem,
    up_here,
    first_here,
):
    tp, x = lax.axis_index("tp"), lax.axis_index("seq")
    ranks, nx = lax.axis_size("tp"), lax.axis_size("seq")
    fan = ranks // KVH
    chips = fan // CORES
    rank = lax.rem(tp, fan)
    z, core = rank // CORES, lax.rem(tp, CORES)
    layers, pages = kv.shape[1], kv.shape[3]
    pieces = [(kind, layer) for kind in range(kv.shape[0]) for layer in range(layers)]
    last = chips - 1
    both, no = jnp.logical_and, jnp.logical_not
    corner = both(z == 0, x == 0)
    first = both(corner, core == 0)
    stand_in = both(corner, core == 1)
    usual, absent = no(corner), no(first)
    above = both(z == 1, x == 0)
    row = both(z == 0, x > 0)
    pair = {"tp": tp + 1 - 2 * core}
    down = {"tp": tp - CORES + jnp.where(both(above, core == 0), 1, 0)}

    def seq_rank(steps):
        return lax.rem(x + steps + nx, nx)

    def up(of_core):
        return {"tp": tp + CORES + of_core - core}

    def along_seq(steps):
        target = seq_rank(steps)
        aside = jnp.where(both(both(row, core == 0), target == 0), 1, 0)
        return {"tp": tp + aside, "seq": target}

    barrier = pltpu.get_barrier_semaphore()

    def signal(semaphore, device):
        pl.semaphore_signal(semaphore, inc=1, device_id=device, device_id_type=MESH)

    @pl.when(absent)
    def _():
        signal(barrier, pair)
        for step in range(1, nx):
            signal(barrier, along_seq(step))
        pl.when(z < last)(lambda: signal(barrier, up(core)))
        pl.when(both(row, core == 1))(lambda: signal(barrier, {"tp": tp - 1, "seq": 0}))
        pl.when(both(above, core == 1))(lambda: signal(barrier, {"tp": tp - CORES - 1}))

    @pl.when(stand_in)
    def _():
        signal(barrier, up(0))
        for step in range(1, nx):
            signal(barrier, {"tp": tp - 1, "seq": step})

    greetings = jnp.where(first, nx + 1, jnp.where(stand_in, 2 * (nx - 1), nx + jnp.where(z > 0, 1, 0)))
    pl.semaphore_wait(barrier, greetings)
    pl.when(z > 0)(lambda: signal(up_here, down))

    def index(of_core, plane, kind):
        return (of_core * chips + plane) * nx + kind

    def start_of(of_core, plane, kind):
        return ((plane * CORES + of_core) * nx + seq_rank(kind)) * pages

    def place(of_core, plane, kind):
        return cache.at[:, :, pl.ds(start_of(of_core, plane, kind), pages)]

    def remote(src, dst, sent, landed, device):
        return pltpu.make_async_remote_copy(
            src_ref=src, dst_ref=dst, send_sem=sent, recv_sem=landed, device_id=device, device_id_type=MESH
        )

    def moved(sent, landed, device, of_core, plane, kind, src):
        block = place(of_core, plane, kind)
        return remote(block if src is None else src, block, sent, landed, device)

    def to_up(of_core, plane, kind, src=None):
        at = own_sem.at[index(of_core, plane, kind)]
        return moved(up_sent.at[plane], at, up(of_core), of_core, plane, kind, src)

    def to_down(plane, kind, src=None):
        at = own_sem.at[index(core, plane, kind)]
        return moved(down_sent.at[plane], at, down, core, plane, kind, src)

    def to_pair(plane, kind, src=None):
        return moved(pair_sent.at[plane], pair_sem.at[plane], pair, core, plane, kind, src)

    def to_first_one(of_core, plane, kind):
        return moved(bulk_sent, bulk_sem, pair, of_core, plane, kind, None)

    def blocks(count, semaphore):
        every = cache.at[:, :, pl.ds(0, count * pages)]
        return remote(every, every, semaphore, semaphore, pair)

    def to_seq(kind):
        start = ((z * CORES + core) * nx + x) * pages
        return remote(
            kv.at[:, :, seq_rank(-kind)],
            cache.at[:, :, pl.ds(start, pages)],
            x_sent,
            own_sem.at[index(core, z, kind)],
            along_seq(-kind),
        )

    def first_piece(piece):
        kind, layer = pieces[piece]
        start = start_of(0, 0, lax.rem(nx - x, nx))
        return cache.at[kind, layer, pl.ds(start, pages)]

    def first_to(steps, piece, device):
        kind, layer = pieces[piece]
        return remote(
            kv.at[kind, layer, steps],
            cache.at[kind, layer, pl.ds(0, pages)],
            first_sent,
            first_sem.at[piece],
            device,
        )

    def first_up(piece):
        block = first_piece(piece)
        return remote(block, block, first_up_sent, first_sem.at[piece], up(core))

    def first_pair(piece):
        block = first_piece(piece)
        return remote(block, block, first_pair_sent, first_pair_sem, pair)

    kinds = [0, *sorted(range(1, nx), key=lambda k: (min(k, nx - k), k))]
    mine = kv.at[:, :, x]

    @pl.when(first)
    def _():
        signal(first_here, pair)
        away = [(k, {"tp": tp + 1, "seq": k}) for k in kinds[1:]]
        for steps, device in [away[-1], (0, {"tp": tp + CORES + 1}), *away[:-1], (0, pair)]:
            for piece in range(len(pieces)):
                first_to(steps, piece, device).start()

    pl.when(z > 0)(lambda: to_down(z, 0, mine).start())

    @pl.when(absent)
    def _():
        for kind in kinds[1:]:
            to_seq(kind).start()

    pl.when(usual)(lambda: to_pair(z, 0, mine).start())
    local = pltpu.make_async_copy(mine, place(core, z, 0), local_sem)
    local.start()
    small = [(slots, slots_here), (queries, queries_here), (new_kv, new_kv_here)]
    small = [pltpu.make_async_copy(*ends, small_sem.at[at]) for at, ends in enumerate(small)]
    for copy in small:
        copy.start()

    @pl.when(both(absent, z < last))
    def _():
        pl.semaphore_wait(up_here, jnp.where(stand_in, 2, 1))
        to_up(core, z, 0, mine).start()

    def arrive(of_core, plane, kind):
        to_up(of_core, plane, kind).wait_recv()

    def from_first(of_core, plane, kind):
        return both(both(plane == 0, of_core == 0), seq_rank(kind) == 0)

    def own(kind):
        @pl.when(both(absent, no(from_first(core, z, kind))))
        def _():
            arrive(core, z, kind)
            pl.when(z > 0)(lambda: to_down(z, kind).start())
            pl.when(z < last)(lambda: to_up(core, z, kind).start())
            pl.when(usual)(lambda: to_pair(z, kind).start())

        @pl.when(stand_in)
        def _():
            arrive(0, z, kind)
            to_up(0, z, kind).start()

    def passing(hops, kind, first_is_here):
        @pl.when(both(absent, z + hops <= last))
        def _():
            arrive(core, z + hops, kind)
            pl.when(z > 0)(lambda: to_down(z + hops, kind).start())
            pl.when(usual)(lambda: to_pair(z + hops, kind).start())

            @pl.when(stand_in)
            def _():
                arrive(0, hops, kind)
                if first_is_here:
                    to_first_one(0, hops, kind).start()
                    to_first_one(1, hops, kind).start()

        @pl.when(both(z - hops >= 0, no(from_first(core, z - hops, kind))))
        def _():
            arrive(core, z - hops, kind)
            pl.when(z < last)(lambda: to_up(core, z - hops, kind).start())
            to_pair(z - hops, kind).start()

    def pass_first():
        for piece in range(len(pieces)):
            first_up(piece).wait_recv()
            pl.when(both(z < last, usual))(lambda: first_up(piece).start())
            pl.when(usual)(lambda: first_pair(piece).start())

    def to_first(piece):
        kind, layer = pieces[piece]
        block = cache.at[kind, layer, pl.ds(pages, (last * CORES * nx - 1) * pages)]
        return remote(block, block, bulk_sent, bulk_sem, pair)

    order = arrival_order(chips, kinds)
    for kind in kinds[1:-1]:
        own(kind)
    near = max(at for at, (hops, _) in enumerate(order) if hops < last)
    for at, (hops, kind) in enumerate(order):
        passing(hops, kind, at > near)
        if at == 0:
            own(kinds[-1])
        if at == near:

            @pl.when(stand_in)
            def _():
                local.wait()
                pl.semaphore_wait(first_here, 1)
                for piece in range(len(pieces)):
                    to_first(piece).start()
                for far, of_kind in order[:at]:
                    if far == last:
                        to_first_one(0, far, of_kind).start()
                        to_first_one(1, far, of_kind).start()

        if at == len(order) - 3:
            pl.when(both(row, core == 1))(pass_first)
    for copy in small:
        copy.wait()
    pl.when(no(stand_in))(lambda: local.wait())
    pl.when(absent)(lambda: blocks(nx - 1, x_sent).wait_send())

    @pl.when(usual)
    def _():
        for plane in range(1, chips):
            blocks(nx, pair_sem.at[plane]).wait_recv()
            blocks(nx, pair_sent.at[plane]).wait_send()

        @pl.when(core == 0)
        def _():
            blocks(nx, pair_sem.at[0]).wait_recv()
            blocks(nx - 1, pair_sent.at[0]).wait_send()

        @pl.when(core == 1)
        def _():
            blocks(nx - 1, pair_sem.at[0]).wait_recv()
            blocks(nx, pair_sent.at[0]).wait_send()

    pl.when(both(jnp.logical_or(z > 0, stand_in), core == 1))(pass_first)

    for plane in range(chips):
        pl.when(both(z > 0, plane >= z))(lambda: blocks(nx, down_sent.at[plane]).wait_send())
    for plane in range(1, last):
        pl.when(both(z < last, plane <= z))(lambda: blocks(nx, up_sent.at[plane]).wait_send())
    below = both(usual, z < last)
    pl.when(both(below, core == 0))(lambda: blocks(nx - 1, up_sent.at[0]).wait_send())
    pl.when(both(below, core == 1))(lambda: blocks(nx, up_sent.at[0]).wait_send())
    pl.when(both(below, core == 1))(lambda: blocks(1, first_up_sent).wait_send())
    pl.when(both(usual, core == 1))(lambda: blocks(1, first_pair_sent).wait_send())
    pl.when(both(usual, core == 0))(lambda: blocks(1, first_pair_sem).wait_recv())
    handed = chips * CORES * nx - 1

    @pl.when(stand_in)
    def _():
        blocks(2 * nx - 1, up_sent.at[0]).wait_send()
        blocks(handed, bulk_sent).wait_send()

    @pl.when(first)
    def _():
        blocks(nx + 1, first_sent).wait_send()
        blocks(handed, bulk_sem).wait_recv()


def attend(length, queries, cache, fresh):
    layers, head = queries.shape
    scale = 1.0 / math.sqrt(head)
    every = range(layers)
    keys = [cache[0, layer].reshape(CTX, head) for layer in every]
    values = [cache[1, layer].reshape(CTX, head) for layer in every]
    q = [jnp.broadcast_to(queries[layer : layer + 1], (8, head)) for layer in every]
    contract = (((1,), (1,)), ((), ()))
    scores = [lax.dot_general(q[i], keys[i], contract, preferred_element_type=jnp.float32) * scale for i in every]
    new = [jnp.sum(q[i].astype(jnp.float32) * fresh(0, i), axis=1, keepdims=True) * scale for i in every]
    visible = lax.broadcasted_iota(jnp.int32, scores[0].shape, 1) < length
    scores = [jnp.where(visible, s, -1e30) for s in scores]
    top = [jnp.maximum(jnp.max(s, axis=1, keepdims=True), n) for s, n in zip(scores, new)]
    weights = [jnp.where(visible, jnp.exp(s - t), 0.0) for s, t in zip(scores, top)]
    new = [jnp.exp(n - t) for n, t in zip(new, top)]
    total = [jnp.sum(w, axis=1, keepdims=True) + n for w, n in zip(weights, new)]
    mixed = [jnp.dot(weights[i].astype(values[i].dtype), values[i], preferred_element_type=jnp.float32) for i in every]
    return [(mixed[i] + new[i] * fresh(1, i)) / total[i] for i in every]


def page_kernel(lengths, slots, cache, queries, new_kv, pool, out, tile, sem, tile_sem):
    kinds, layers, pages, head = cache.shape[0], cache.shape[1], cache.shape[2], cache.shape[4]
    length = lengths[0]
    page_now, row_now = length // PAGE, lax.rem(length, PAGE)
    head_now = lax.axis_index("tp") * KVH // lax.axis_size("tp")
    rows = lax.broadcasted_iota(jnp.int32, (PAGE, head), 0)

    def place(page):
        return pool.at[:, :, 0, slots[0, page]]

    def put(step, _):
        page = lax.rem(page_now + step, pages)
        pltpu.make_async_copy(cache.at[:, :, page], place(page), sem).start()
        return 0

    lax.fori_loop(1, pages, put, 0, unroll=15)

    def fresh(kind, layer):
        block = new_kv[kind, layer, 0].astype(jnp.float32)
        mine = lax.broadcasted_iota(jnp.int32, block.shape, 0) == head_now
        return jnp.sum(jnp.where(mine, block, 0.0), axis=0, keepdims=True)

    for kind in range(kinds):
        for layer in range(layers):
            held = cache[kind, layer, page_now].astype(jnp.float32)
            tile[kind, layer] = jnp.where(rows == row_now, fresh(kind, layer), held).astype(tile.dtype)
    placed = pltpu.make_async_copy(tile, place(page_now), tile_sem)
    placed.start()
    for layer, mixed in enumerate(attend(length, queries, cache, fresh)):
        out[layer : layer + 1] = mixed[:1].astype(out.dtype)
    others = pl.ds(1, pages - 1)
    pltpu.make_async_copy(cache.at[:, :, others], pool.at[:, :, 0, others], sem).wait()
    placed.wait()


def body(kv_prefill, queries, new_kv, lengths, page_slots):
    kinds, layers, seqs, positions, head = kv_prefill.shape
    nx = lax.axis_size("seq")
    fan = lax.axis_size("tp") // KVH
    chips = fan // CORES
    pages = CTX // PAGE
    pieces = kinds * layers
    dma = pltpu.SemaphoreType.DMA
    anywhere = pl.BlockSpec(memory_space=pl.ANY)
    vmem = pl.BlockSpec(memory_space=pltpu.VMEM)
    smem = pl.BlockSpec(memory_space=pltpu.SMEM)
    cache_shape = (kinds, layers, pages, PAGE, head)
    blocks = kv_prefill.reshape(kinds, layers, seqs, positions // PAGE, PAGE, head)
    hbm = pl.BlockSpec(memory_space=pltpu.HBM)
    small = (page_slots, queries.reshape(layers, head), new_kv)
    cache, *small = pl.pallas_call(
        spread_kernel,
        out_shape=(
            pltpu.VMEM(cache_shape, kv_prefill.dtype),
            pltpu.SMEM(page_slots.shape, page_slots.dtype),
            pltpu.VMEM((layers, head), queries.dtype),
            pltpu.VMEM(new_kv.shape, new_kv.dtype),
        ),
        in_specs=[hbm] * 4,
        out_specs=(vmem, smem, vmem, vmem),
        scratch_shapes=[
            dma((fan * nx,)),
            dma((chips,)),
            dma((pieces,)),
            dma,
            dma,
            dma,
            dma((chips,)),
            dma((chips,)),
            dma((chips,)),
            dma,
            dma,
            dma,
            dma,
            dma,
            dma((3,)),
            pltpu.SemaphoreType.REGULAR,
            pltpu.SemaphoreType.REGULAR,
        ],
        compiler_params=pltpu.CompilerParams(collective_id=0, has_side_effects=True, vmem_limit_bytes=16 * MIB),
        name="spread",
    )(*(pltpu.with_memory_space_constraint(a, pltpu.HBM) for a in (blocks, *small)))
    pool, out = pl.pallas_call(
        page_kernel,
        out_shape=(
            jax.ShapeDtypeStruct((kinds, layers, 1, pages, PAGE, head), kv_prefill.dtype),
            jax.ShapeDtypeStruct((layers, head), queries.dtype),
        ),
        in_specs=[smem, smem, vmem, vmem, vmem],
        out_specs=(anywhere, vmem),
        scratch_shapes=[pltpu.VMEM((kinds, layers, PAGE, head), kv_prefill.dtype), dma, dma],
        compiler_params=pltpu.CompilerParams(vmem_limit_bytes=24 * MIB),
        name="pages",
    )(lengths, small[0], cache, *small[1:])
    return pool, out.reshape(queries.shape)


def solution(mesh):
    placed = (
        P(None, None, "groups", ("tp", "seq"), None),
        P(None, ("groups", "seq"), "tp", None),
        P(None, None, ("groups", "seq"), None, None),
        P(("groups", "seq")),
        P(("groups", "seq"), None),
    )
    return jax.shard_map(
        body,
        mesh=mesh,
        in_specs=placed,
        out_specs=(
            P(None, None, "tp", ("groups", "seq"), None, None),
            P(None, ("groups", "seq"), "tp", None),
        ),
        check_vma=False,
    )
```

```python
import functools
import math

import jax
import jax.numpy as jnp
from jax import lax
from jax.experimental import pallas as pl
from jax.experimental.pallas import tpu as pltpu
from jax.sharding import PartitionSpec as P

KVH = 8
PAGE = 16
CTX = 4096
CORES = 2
MESH = pl.DeviceIdType.MESH
MIB = 1 << 20


def arrival_order(chips, kinds):
    order = []
    for _ in range(chips - 1):
        further = [(hops + 1, kind) for hops, kind in order]
        own = [(1, kind) for kind in kinds]
        order = own[:-1] + further[:1] + own[-1:] + further[1:]
    return order


def spread_kernel(
    kv,
    slots,
    queries,
    new_kv,
    cache,
    slots_here,
    queries_here,
    new_kv_here,
    own_sem,
    pair_sem,
    first_sem,
    first_pair_sem,
    bulk_sem,
    direct_sem,
    x_sent,
    up_sent,
    down_sent,
    pair_sent,
    first_sent,
    first_up_sent,
    first_pair_sent,
    bulk_sent,
    direct_sent,
    local_sem,
    small_sem,
    up_here,
    first_here,
):
    tp, x = lax.axis_index("tp"), lax.axis_index("seq")
    ranks, nx = lax.axis_size("tp"), lax.axis_size("seq")
    fan = ranks // KVH
    chips = fan // CORES
    rank = lax.rem(tp, fan)
    z, core = rank // CORES, lax.rem(tp, CORES)
    layers, pages = kv.shape[1], kv.shape[3]
    pieces = [(kind, layer) for kind in range(kv.shape[0]) for layer in range(layers)]
    last = chips - 1
    both, no = jnp.logical_and, jnp.logical_not
    corner = both(z == 0, x == 0)
    first = both(corner, core == 0)
    stand_in = both(corner, core == 1)
    usual, absent = no(corner), no(first)
    above = both(z == 1, x == 0)
    row = both(z == 0, x > 0)
    near_row = both(z == 0, jnp.logical_or(x == 1, x == nx - 1))
    helper = jnp.logical_or(near_row, above)
    to_corner = {"tp": tp - z * CORES - core, "seq": 0}
    near = sorted({1, nx - 1})
    pair = {"tp": tp + 1 - 2 * core}
    down = {"tp": tp - CORES + jnp.where(both(above, core == 0), 1, 0)}

    def seq_rank(steps):
        return lax.rem(x + steps + nx, nx)

    def up(of_core):
        return {"tp": tp + CORES + of_core - core}

    def along_seq(steps):
        target = seq_rank(steps)
        aside = jnp.where(both(both(row, core == 0), target == 0), 1, 0)
        return {"tp": tp + aside, "seq": target}

    barrier = pltpu.get_barrier_semaphore()

    def signal(semaphore, device):
        pl.semaphore_signal(semaphore, inc=1, device_id=device, device_id_type=MESH)

    @pl.when(absent)
    def _():
        signal(barrier, pair)
        for step in range(1, nx):
            signal(barrier, along_seq(step))
        pl.when(z < last)(lambda: signal(barrier, up(core)))
        pl.when(jnp.logical_or(helper, both(row, core == 1)))(lambda: signal(barrier, to_corner))

    @pl.when(stand_in)
    def _():
        signal(barrier, up(0))
        for step in range(1, nx):
            signal(barrier, {"tp": tp - 1, "seq": step})

    greetings = jnp.where(first, nx + 2 + len(near), jnp.where(stand_in, 2 * (nx - 1), nx + jnp.where(z > 0, 1, 0)))
    pl.semaphore_wait(barrier, greetings)
    pl.when(z > 0)(lambda: signal(up_here, down))

    def index(of_core, plane, kind):
        return (of_core * chips + plane) * nx + kind

    def start_of(of_core, plane, kind):
        return ((plane * CORES + of_core) * nx + seq_rank(kind)) * pages

    def place(of_core, plane, kind):
        return cache.at[:, :, pl.ds(start_of(of_core, plane, kind), pages)]

    def remote(src, dst, sent, landed, device):
        return pltpu.make_async_remote_copy(
            src_ref=src, dst_ref=dst, send_sem=sent, recv_sem=landed, device_id=device, device_id_type=MESH
        )

    def moved(sent, landed, device, of_core, plane, kind, src):
        block = place(of_core, plane, kind)
        return remote(block if src is None else src, block, sent, landed, device)

    def to_up(of_core, plane, kind, src=None):
        at = own_sem.at[index(of_core, plane, kind)]
        return moved(up_sent.at[plane], at, up(of_core), of_core, plane, kind, src)

    def to_down(plane, kind, src=None):
        at = own_sem.at[index(core, plane, kind)]
        return moved(down_sent.at[plane], at, down, core, plane, kind, src)

    def to_pair(plane, kind, src=None):
        return moved(pair_sent.at[plane], pair_sem.at[plane], pair, core, plane, kind, src)

    def to_first_one(of_core, plane, kind):
        return moved(bulk_sent, bulk_sem, pair, of_core, plane, kind, None)

    def blocks(count, semaphore):
        every = cache.at[:, :, pl.ds(0, count * pages)]
        return remote(every, every, semaphore, semaphore, pair)

    def to_seq(kind):
        start = ((z * CORES + core) * nx + x) * pages
        return remote(
            kv.at[:, :, seq_rank(-kind)],
            cache.at[:, :, pl.ds(start, pages)],
            x_sent,
            own_sem.at[index(core, z, kind)],
            along_seq(-kind),
        )

    def first_piece(piece):
        kind, layer = pieces[piece]
        start = start_of(0, 0, lax.rem(nx - x, nx))
        return cache.at[kind, layer, pl.ds(start, pages)]

    def first_to(steps, piece, device):
        kind, layer = pieces[piece]
        return remote(
            kv.at[kind, layer, steps],
            cache.at[kind, layer, pl.ds(0, pages)],
            first_sent,
            first_sem.at[piece],
            device,
        )

    def first_up(piece):
        block = first_piece(piece)
        return remote(block, block, first_up_sent, first_sem.at[piece], up(core))

    def first_pair(piece):
        block = first_piece(piece)
        return remote(block, block, first_pair_sent, first_pair_sem, pair)

    kinds = [0, *sorted(range(1, nx), key=lambda k: (min(k, nx - k), k))]
    mine = kv.at[:, :, x]

    @pl.when(first)
    def _():
        signal(first_here, pair)
        for of_core in range(CORES):
            signal(first_here, {"tp": tp + CORES + of_core})
            for k in near:
                signal(first_here, {"tp": tp + of_core, "seq": k})
        away = [(k, {"tp": tp + 1, "seq": k}) for k in kinds[1:]]
        for steps, device in [away[-1], (0, {"tp": tp + CORES + 1}), *away[:-1], (0, pair)]:
            for piece in range(len(pieces)):
                first_to(steps, piece, device).start()

    pl.when(z > 0)(lambda: to_down(z, 0, mine).start())

    @pl.when(absent)
    def _():
        for kind in kinds[1:]:
            to_seq(kind).start()

    pl.when(usual)(lambda: to_pair(z, 0, mine).start())
    local = pltpu.make_async_copy(mine, place(core, z, 0), local_sem)
    local.start()
    small = [(slots, slots_here), (queries, queries_here), (new_kv, new_kv_here)]
    small = [pltpu.make_async_copy(*ends, small_sem.at[at]) for at, ends in enumerate(small)]
    for copy in small:
        copy.start()

    @pl.when(both(absent, z < last))
    def _():
        pl.semaphore_wait(up_here, jnp.where(stand_in, 2, 1))
        to_up(core, z, 0, mine).start()

    def arrive(of_core, plane, kind):
        to_up(of_core, plane, kind).wait_recv()

    def from_first(of_core, plane, kind):
        return both(both(plane == 0, of_core == 0), seq_rank(kind) == 0)

    def own(kind):
        @pl.when(both(absent, no(from_first(core, z, kind))))
        def _():
            arrive(core, z, kind)
            pl.when(z > 0)(lambda: to_down(z, kind).start())
            pl.when(z < last)(lambda: to_up(core, z, kind).start())
            pl.when(usual)(lambda: to_pair(z, kind).start())

        @pl.when(stand_in)
        def _():
            arrive(0, z, kind)
            to_up(0, z, kind).start()

    def passing(hops, kind, first_is_here):
        @pl.when(both(absent, z + hops <= last))
        def _():
            arrive(core, z + hops, kind)
            pl.when(z > 0)(lambda: to_down(z + hops, kind).start())
            pl.when(usual)(lambda: to_pair(z + hops, kind).start())

            @pl.when(stand_in)
            def _():
                arrive(0, hops, kind)
                if first_is_here and kind != kinds[-1]:
                    to_first_one(0, hops, kind).start()
                    to_first_one(1, hops, kind).start()

        @pl.when(both(z - hops >= 0, no(from_first(core, z - hops, kind))))
        def _():
            arrive(core, z - hops, kind)
            pl.when(z < last)(lambda: to_up(core, z - hops, kind).start())
            to_pair(z - hops, kind).start()

    def pass_first():
        for piece in range(len(pieces)):
            first_up(piece).wait_recv()
            pl.when(both(z < last, usual))(lambda: first_up(piece).start())
            pl.when(usual)(lambda: first_pair(piece).start())

    def to_first(piece):
        kind, layer = pieces[piece]
        block = cache.at[kind, layer, pl.ds(CORES * nx * pages, (last - 1) * CORES * nx * pages)]
        return remote(block, block, bulk_sent, bulk_sem, pair)

    def direct(of_core, of_x, src=None):
        plane = 0 if of_x else last
        of_seq = of_x if of_x else kinds[-1]
        block = cache.at[:, :, pl.ds(((plane * CORES + of_core) * nx + of_seq) * pages, pages)]
        landed = direct_sem.at[of_core * nx + of_x]
        return remote(block if src is None else src, block, direct_sent, landed, to_corner)

    def help_row():
        pl.semaphore_wait(first_here, 1)
        for of_core in range(CORES):
            for k in near:
                pl.when(both(core == of_core, x == k))(
                    lambda of_core=of_core, k=k: direct(of_core, k, kv.at[:, :, 0]).start()
                )

    def help_above():
        pl.semaphore_wait(first_here, 1)
        for of_core in range(CORES):
            pl.when(core == of_core)(lambda of_core=of_core: direct(of_core, 0).start())

    order = arrival_order(chips, kinds)
    for kind in kinds[1:-1]:
        own(kind)
    middle = max(at for at, (hops, _) in enumerate(order) if hops < last)
    for at, (hops, kind) in enumerate(order):
        passing(hops, kind, at > middle)
        if at == 0:
            own(kinds[-1])
        if at == middle:

            @pl.when(stand_in)
            def _():
                local.wait()
                pl.semaphore_wait(first_here, 1)
                for piece in range(len(pieces)):
                    to_first(piece).start()
                for of_core, of_seq in [(of_core, k) for of_core in range(CORES) for k in kinds]:
                    if of_seq not in near and (of_core, of_seq) != (0, 0):
                        to_first_one(of_core, 0, of_seq).start()
                for far, of_kind in order[:at]:
                    if far == last and of_kind != kinds[-1]:
                        to_first_one(0, far, of_kind).start()
                        to_first_one(1, far, of_kind).start()

        if at == len(order) - 3:
            pl.when(both(row, core == 1))(pass_first)
            pl.when(near_row)(help_row)
    pl.when(above)(help_above)
    for copy in small:
        copy.wait()
    pl.when(no(stand_in))(lambda: local.wait())
    pl.when(absent)(lambda: blocks(nx - 1, x_sent).wait_send())

    @pl.when(usual)
    def _():
        for plane in range(1, chips):
            blocks(nx, pair_sem.at[plane]).wait_recv()
            blocks(nx, pair_sent.at[plane]).wait_send()

        @pl.when(core == 0)
        def _():
            blocks(nx, pair_sem.at[0]).wait_recv()
            blocks(nx - 1, pair_sent.at[0]).wait_send()

        @pl.when(core == 1)
        def _():
            blocks(nx - 1, pair_sem.at[0]).wait_recv()
            blocks(nx, pair_sent.at[0]).wait_send()

    pl.when(both(jnp.logical_or(z > 0, stand_in), core == 1))(pass_first)

    for plane in range(chips):
        pl.when(both(z > 0, plane >= z))(lambda: blocks(nx, down_sent.at[plane]).wait_send())
    for plane in range(1, last):
        pl.when(both(z < last, plane <= z))(lambda: blocks(nx, up_sent.at[plane]).wait_send())
    below = both(usual, z < last)
    pl.when(both(below, core == 0))(lambda: blocks(nx - 1, up_sent.at[0]).wait_send())
    pl.when(both(below, core == 1))(lambda: blocks(nx, up_sent.at[0]).wait_send())
    pl.when(both(below, core == 1))(lambda: blocks(1, first_up_sent).wait_send())
    pl.when(both(usual, core == 1))(lambda: blocks(1, first_pair_sent).wait_send())
    pl.when(both(usual, core == 0))(lambda: blocks(1, first_pair_sem).wait_recv())
    handed = chips * CORES * nx - 1 - CORES * (len(near) + 1)
    pl.when(helper)(lambda: blocks(1, direct_sent).wait_send())

    @pl.when(stand_in)
    def _():
        blocks(2 * nx - 1, up_sent.at[0]).wait_send()
        blocks(handed, bulk_sent).wait_send()

    @pl.when(first)
    def _():
        blocks(nx + 1, first_sent).wait_send()
        blocks(handed, bulk_sem).wait_recv()
        for of_core in range(CORES):
            for of_x in [0, *near]:
                direct(of_core, of_x).wait_recv()


def attend(length, queries, cache, fresh):
    layers, head = queries.shape
    scale = 1.0 / math.sqrt(head)
    every = range(layers)
    keys = [cache[0, layer].reshape(CTX, head) for layer in every]
    values = [cache[1, layer].reshape(CTX, head) for layer in every]
    q = [jnp.broadcast_to(queries[layer : layer + 1], (8, head)) for layer in every]
    contract = (((1,), (1,)), ((), ()))
    scores = [lax.dot_general(q[i], keys[i], contract, preferred_element_type=jnp.float32) * scale for i in every]
    new = [jnp.sum(q[i].astype(jnp.float32) * fresh(0, i), axis=1, keepdims=True) * scale for i in every]
    visible = lax.broadcasted_iota(jnp.int32, scores[0].shape, 1) < length
    scores = [jnp.where(visible, s, -1e30) for s in scores]
    top = [jnp.maximum(jnp.max(s, axis=1, keepdims=True), n) for s, n in zip(scores, new)]
    weights = [jnp.where(visible, jnp.exp(s - t), 0.0) for s, t in zip(scores, top)]
    new = [jnp.exp(n - t) for n, t in zip(new, top)]
    total = [jnp.sum(w, axis=1, keepdims=True) + n for w, n in zip(weights, new)]
    mixed = [jnp.dot(weights[i].astype(values[i].dtype), values[i], preferred_element_type=jnp.float32) for i in every]
    return [(mixed[i] + new[i] * fresh(1, i)) / total[i] for i in every]


def page_kernel(lengths, slots, cache, queries, new_kv, pool, out, tile, sem, tile_sem):
    kinds, layers, pages, head = cache.shape[0], cache.shape[1], cache.shape[2], cache.shape[4]
    length = lengths[0]
    page_now, row_now = length // PAGE, lax.rem(length, PAGE)
    head_now = lax.axis_index("tp") * KVH // lax.axis_size("tp")
    rows = lax.broadcasted_iota(jnp.int32, (PAGE, head), 0)

    def place(page):
        return pool.at[:, :, 0, slots[0, page]]

    def put(step, _):
        page = lax.rem(page_now + step, pages)
        pltpu.make_async_copy(cache.at[:, :, page], place(page), sem).start()
        return 0

    looped = 135
    lax.fori_loop(1, looped + 1, put, 0, unroll=15)
    for step in range(looped + 1, pages):
        put(step, 0)

    def fresh(kind, layer):
        block = new_kv[kind, layer, 0].astype(jnp.float32)
        mine = lax.broadcasted_iota(jnp.int32, block.shape, 0) == head_now
        return jnp.sum(jnp.where(mine, block, 0.0), axis=0, keepdims=True)

    for kind in range(kinds):
        for layer in range(layers):
            held = cache[kind, layer, page_now].astype(jnp.float32)
            tile[kind, layer] = jnp.where(rows == row_now, fresh(kind, layer), held).astype(tile.dtype)
    placed = pltpu.make_async_copy(tile, place(page_now), tile_sem)
    placed.start()
    for layer, mixed in enumerate(attend(length, queries, cache, fresh)):
        out[layer : layer + 1] = mixed[:1].astype(out.dtype)
    others = pl.ds(1, pages - 1)
    pltpu.make_async_copy(cache.at[:, :, others], pool.at[:, :, 0, others], sem).wait()
    placed.wait()


def body(kv_prefill, queries, new_kv, lengths, page_slots):
    kinds, layers, seqs, positions, head = kv_prefill.shape
    nx = lax.axis_size("seq")
    fan = lax.axis_size("tp") // KVH
    chips = fan // CORES
    pages = CTX // PAGE
    pieces = kinds * layers
    dma = pltpu.SemaphoreType.DMA
    anywhere = pl.BlockSpec(memory_space=pl.ANY)
    vmem = pl.BlockSpec(memory_space=pltpu.VMEM)
    smem = pl.BlockSpec(memory_space=pltpu.SMEM)
    cache_shape = (kinds, layers, pages, PAGE, head)
    blocks = kv_prefill.reshape(kinds, layers, seqs, positions // PAGE, PAGE, head)
    hbm = pl.BlockSpec(memory_space=pltpu.HBM)
    small = (page_slots, queries.reshape(layers, head), new_kv)
    cache, *small = pl.pallas_call(
        spread_kernel,
        out_shape=(
            pltpu.VMEM(cache_shape, kv_prefill.dtype),
            pltpu.SMEM(page_slots.shape, page_slots.dtype),
            pltpu.VMEM((layers, head), queries.dtype),
            pltpu.VMEM(new_kv.shape, new_kv.dtype),
        ),
        in_specs=[hbm] * 4,
        out_specs=(vmem, smem, vmem, vmem),
        scratch_shapes=[
            dma((fan * nx,)),
            dma((chips,)),
            dma((pieces,)),
            dma,
            dma,
            dma((CORES * nx,)),
            dma,
            dma((chips,)),
            dma((chips,)),
            dma((chips,)),
            dma,
            dma,
            dma,
            dma,
            dma,
            dma,
            dma((3,)),
            pltpu.SemaphoreType.REGULAR,
            pltpu.SemaphoreType.REGULAR,
        ],
        compiler_params=pltpu.CompilerParams(collective_id=0, has_side_effects=True, vmem_limit_bytes=16 * MIB),
        name="spread",
    )(*(pltpu.with_memory_space_constraint(a, pltpu.HBM) for a in (blocks, *small)))
    pool, out = pl.pallas_call(
        page_kernel,
        out_shape=(
            jax.ShapeDtypeStruct((kinds, layers, 1, pages, PAGE, head), kv_prefill.dtype),
            jax.ShapeDtypeStruct((layers, head), queries.dtype),
        ),
        in_specs=[smem, smem, vmem, vmem, vmem],
        out_specs=(anywhere, vmem),
        scratch_shapes=[pltpu.VMEM((kinds, layers, PAGE, head), kv_prefill.dtype), dma, dma],
        compiler_params=pltpu.CompilerParams(vmem_limit_bytes=24 * MIB),
        name="pages",
    )(lengths, small[0], cache, *small[1:])
    return pool, out.reshape(queries.shape)


def solution(mesh):
    placed = (
        P(None, None, "groups", ("tp", "seq"), None),
        P(None, ("groups", "seq"), "tp", None),
        P(None, None, ("groups", "seq"), None, None),
        P(("groups", "seq")),
        P(("groups", "seq"), None),
    )
    return jax.shard_map(
        body,
        mesh=mesh,
        in_specs=placed,
        out_specs=(
            P(None, None, "tp", ("groups", "seq"), None, None),
            P(None, ("groups", "seq"), "tp", None),
        ),
        check_vma=False,
    )
```

```python
import functools
import math

import jax
import jax.numpy as jnp
from jax import lax
from jax.experimental import pallas as pl
from jax.experimental.pallas import tpu as pltpu
from jax.sharding import PartitionSpec as P

KVH = 8
PAGE = 16
CTX = 4096
CORES = 2
MESH = pl.DeviceIdType.MESH
MIB = 1 << 20


def arrival_order(chips, kinds):
    order = []
    for _ in range(chips - 1):
        further = [(hops + 1, kind) for hops, kind in order]
        own = [(1, kind) for kind in kinds]
        order = own[:-1] + further[:1] + own[-1:] + further[1:]
    return order


def spread_kernel(
    kv,
    slots,
    queries,
    new_kv,
    cache,
    slots_here,
    queries_here,
    new_kv_here,
    own_sem,
    pair_sem,
    first_sem,
    first_pair_sem,
    bulk_sem,
    direct_sem,
    relay_sem,
    x_sent,
    up_sent,
    down_sent,
    pair_sent,
    first_sent,
    first_up_sent,
    first_pair_sent,
    bulk_sent,
    direct_sent,
    relay_sent,
    local_sem,
    small_sem,
    up_here,
    first_here,
    relayed,
):
    tp, x = lax.axis_index("tp"), lax.axis_index("seq")
    ranks, nx = lax.axis_size("tp"), lax.axis_size("seq")
    fan = ranks // KVH
    chips = fan // CORES
    rank = lax.rem(tp, fan)
    z, core = rank // CORES, lax.rem(tp, CORES)
    layers, pages = kv.shape[1], kv.shape[3]
    pieces = [(kind, layer) for kind in range(kv.shape[0]) for layer in range(layers)]
    last = chips - 1
    both, no = jnp.logical_and, jnp.logical_not
    corner = both(z == 0, x == 0)
    first = both(corner, core == 0)
    stand_in = both(corner, core == 1)
    usual, absent = no(corner), no(first)
    above = both(z == 1, x == 0)
    row = both(z == 0, x > 0)
    helper = jnp.logical_or(row, above)
    to_corner = {"tp": tp - z * CORES - core, "seq": 0}
    others = range(1, nx)
    relays = both(both(z == 0, x == nx - 1), core == 1)
    pair = {"tp": tp + 1 - 2 * core}
    down = {"tp": tp - CORES + jnp.where(both(above, core == 0), 1, 0)}

    def seq_rank(steps):
        return lax.rem(x + steps + nx, nx)

    def up(of_core):
        return {"tp": tp + CORES + of_core - core}

    def along_seq(steps):
        target = seq_rank(steps)
        aside = jnp.where(both(both(row, core == 0), target == 0), 1, 0)
        return {"tp": tp + aside, "seq": target}

    barrier = pltpu.get_barrier_semaphore()

    def signal(semaphore, device):
        pl.semaphore_signal(semaphore, inc=1, device_id=device, device_id_type=MESH)

    @pl.when(absent)
    def _():
        signal(barrier, pair)
        for step in range(1, nx):
            signal(barrier, along_seq(step))
        pl.when(z < last)(lambda: signal(barrier, up(core)))
        pl.when(helper)(lambda: signal(barrier, to_corner))

    @pl.when(stand_in)
    def _():
        signal(barrier, up(0))
        for step in range(1, nx):
            signal(barrier, {"tp": tp - 1, "seq": step})

    greetings = jnp.where(first, 2 * nx + 1, jnp.where(stand_in, 2 * (nx - 1), nx + jnp.where(z > 0, 1, 0)))
    pl.semaphore_wait(barrier, greetings)
    pl.when(z > 0)(lambda: signal(up_here, down))

    def index(of_core, plane, kind):
        return (of_core * chips + plane) * nx + kind

    def start_of(of_core, plane, kind):
        return ((plane * CORES + of_core) * nx + seq_rank(kind)) * pages

    def place(of_core, plane, kind):
        return cache.at[:, :, pl.ds(start_of(of_core, plane, kind), pages)]

    def remote(src, dst, sent, landed, device):
        return pltpu.make_async_remote_copy(
            src_ref=src, dst_ref=dst, send_sem=sent, recv_sem=landed, device_id=device, device_id_type=MESH
        )

    def moved(sent, landed, device, of_core, plane, kind, src):
        block = place(of_core, plane, kind)
        return remote(block if src is None else src, block, sent, landed, device)

    def to_up(of_core, plane, kind, src=None):
        at = own_sem.at[index(of_core, plane, kind)]
        return moved(up_sent.at[plane], at, up(of_core), of_core, plane, kind, src)

    def to_down(plane, kind, src=None):
        at = own_sem.at[index(core, plane, kind)]
        return moved(down_sent.at[plane], at, down, core, plane, kind, src)

    def to_pair(plane, kind, src=None):
        return moved(pair_sent.at[plane], pair_sem.at[plane], pair, core, plane, kind, src)

    def to_first_one(of_core, plane, kind):
        return moved(bulk_sent, bulk_sem, pair, of_core, plane, kind, None)

    def blocks(count, semaphore):
        every = cache.at[:, :, pl.ds(0, count * pages)]
        return remote(every, every, semaphore, semaphore, pair)

    def to_seq(kind):
        start = ((z * CORES + core) * nx + x) * pages
        return remote(
            kv.at[:, :, seq_rank(-kind)],
            cache.at[:, :, pl.ds(start, pages)],
            x_sent,
            own_sem.at[index(core, z, kind)],
            along_seq(-kind),
        )

    kinds = [0, *sorted(range(1, nx), key=lambda k: (min(k, nx - k), k))]

    def first_piece(piece):
        kind, layer = pieces[piece]
        start = start_of(0, 0, lax.rem(nx - x, nx))
        return cache.at[kind, layer, pl.ds(start, pages)]

    def first_to(steps, piece, device):
        kind, layer = pieces[piece]
        return remote(
            kv.at[kind, layer, steps],
            cache.at[kind, layer, pl.ds(0, pages)],
            first_sent,
            first_sem.at[piece],
            device,
        )

    half, far = len(pieces) // 2, kinds[-1]

    def first_relay(at):
        kind, layer = pieces[half + at]
        by = {"tp": tp + 1, "seq": nx - 1}
        return remote(kv.at[kind, layer, far], relayed.at[at], first_sent, relay_sem.at[at], by)

    def relay_on(at):
        kind, layer = pieces[half + at]
        block = cache.at[kind, layer, pl.ds(0, pages)]
        return remote(relayed.at[at], block, relay_sent, first_sem.at[half + at], {"seq": far})

    def relay():
        for at in range(half):
            first_relay(at).wait_recv()
            relay_on(at).start()

    def first_up(piece):
        block = first_piece(piece)
        return remote(block, block, first_up_sent, first_sem.at[piece], up(core))

    def first_pair(piece):
        block = first_piece(piece)
        return remote(block, block, first_pair_sent, first_pair_sem, pair)

    mine = kv.at[:, :, x]

    @pl.when(first)
    def _():
        signal(first_here, pair)
        for of_core in range(CORES):
            signal(first_here, {"tp": tp + CORES + of_core})
            for k in others:
                signal(first_here, {"tp": tp + of_core, "seq": k})
        every = range(len(pieces))
        sends = [(k, piece) for piece in every[:half] for k in (far, *kinds[1:-1], 0)]
        sends += [(k, piece) for piece in every[half:] for k in (*kinds[1:-1], 0)]
        for at in range(half):
            first_relay(at).start()
        for k, piece in sends:
            first_to(k, piece, {"tp": tp + (1 if k else CORES + 1), "seq": k}).start()
        for piece in every:
            first_to(0, piece, pair).start()

    pl.when(z > 0)(lambda: to_down(z, 0, mine).start())

    @pl.when(absent)
    def _():
        for kind in kinds[1:]:
            to_seq(kind).start()

    pl.when(usual)(lambda: to_pair(z, 0, mine).start())
    local = pltpu.make_async_copy(mine, place(core, z, 0), local_sem)
    local.start()
    small = [(slots, slots_here), (queries, queries_here), (new_kv, new_kv_here)]
    small = [pltpu.make_async_copy(*ends, small_sem.at[at]) for at, ends in enumerate(small)]
    for copy in small:
        copy.start()

    @pl.when(both(absent, z < last))
    def _():
        pl.semaphore_wait(up_here, jnp.where(stand_in, 2, 1))
        to_up(core, z, 0, mine).start()

    def arrive(of_core, plane, kind):
        to_up(of_core, plane, kind).wait_recv()

    def from_first(of_core, plane, kind):
        return both(both(plane == 0, of_core == 0), seq_rank(kind) == 0)

    def own(kind):
        @pl.when(both(absent, no(from_first(core, z, kind))))
        def _():
            arrive(core, z, kind)
            pl.when(z > 0)(lambda: to_down(z, kind).start())
            pl.when(z < last)(lambda: to_up(core, z, kind).start())
            pl.when(usual)(lambda: to_pair(z, kind).start())

        @pl.when(stand_in)
        def _():
            arrive(0, z, kind)
            to_up(0, z, kind).start()

    def passing(hops, kind, first_is_here):
        @pl.when(both(absent, z + hops <= last))
        def _():
            arrive(core, z + hops, kind)
            pl.when(z > 0)(lambda: to_down(z + hops, kind).start())
            pl.when(usual)(lambda: to_pair(z + hops, kind).start())

            @pl.when(stand_in)
            def _():
                arrive(0, hops, kind)
                if first_is_here and kind != kinds[-1]:
                    to_first_one(0, hops, kind).start()
                    to_first_one(1, hops, kind).start()

        @pl.when(both(z - hops >= 0, no(from_first(core, z - hops, kind))))
        def _():
            arrive(core, z - hops, kind)
            pl.when(z < last)(lambda: to_up(core, z - hops, kind).start())
            to_pair(z - hops, kind).start()

    def pass_first():
        for piece in range(len(pieces)):
            first_up(piece).wait_recv()
            pl.when(both(z < last, usual))(lambda: first_up(piece).start())
            pl.when(usual)(lambda: first_pair(piece).start())

    def to_first(piece):
        kind, layer = pieces[piece]
        block = cache.at[kind, layer, pl.ds(CORES * nx * pages, (last - 1) * CORES * nx * pages)]
        return remote(block, block, bulk_sent, bulk_sem, pair)

    def direct(of_core, of_x, src=None):
        plane = 0 if of_x else last
        of_seq = of_x if of_x else kinds[-1]
        block = cache.at[:, :, pl.ds(((plane * CORES + of_core) * nx + of_seq) * pages, pages)]
        landed = direct_sem.at[of_core * nx + of_x]
        return remote(block if src is None else src, block, direct_sent, landed, to_corner)

    def help_row():
        pl.semaphore_wait(first_here, 1)
        for of_core in range(CORES):
            for k in others:
                pl.when(both(core == of_core, x == k))(
                    lambda of_core=of_core, k=k: direct(of_core, k, kv.at[:, :, 0]).start()
                )

    def help_above():
        pl.semaphore_wait(first_here, 1)
        for of_core in range(CORES):
            pl.when(core == of_core)(lambda of_core=of_core: direct(of_core, 0).start())

    order = arrival_order(chips, kinds)
    for kind in kinds[1:-1]:
        own(kind)
    middle = max(at for at, (hops, _) in enumerate(order) if hops < last)
    for at, (hops, kind) in enumerate(order):
        passing(hops, kind, at > middle)
        if at == 0:
            own(kinds[-1])
        if at == middle:

            @pl.when(stand_in)
            def _():
                local.wait()
                pl.semaphore_wait(first_here, 1)
                for piece in range(len(pieces)):
                    to_first(piece).start()
                to_first_one(1, 0, 0).start()
                for far, of_kind in order[:at]:
                    if far == last and of_kind != kinds[-1]:
                        to_first_one(0, far, of_kind).start()
                        to_first_one(1, far, of_kind).start()

        if at == len(order) - 3:
            pl.when(row)(help_row)
            pl.when(relays)(relay)
            pl.when(both(row, core == 1))(pass_first)
    pl.when(above)(help_above)
    for copy in small:
        copy.wait()
    pl.when(no(stand_in))(lambda: local.wait())
    pl.when(absent)(lambda: blocks(nx - 1, x_sent).wait_send())

    @pl.when(usual)
    def _():
        for plane in range(1, chips):
            blocks(nx, pair_sem.at[plane]).wait_recv()
            blocks(nx, pair_sent.at[plane]).wait_send()

        @pl.when(core == 0)
        def _():
            blocks(nx, pair_sem.at[0]).wait_recv()
            blocks(nx - 1, pair_sent.at[0]).wait_send()

        @pl.when(core == 1)
        def _():
            blocks(nx - 1, pair_sem.at[0]).wait_recv()
            blocks(nx, pair_sent.at[0]).wait_send()

    pl.when(both(jnp.logical_or(z > 0, stand_in), core == 1))(pass_first)

    for plane in range(chips):
        pl.when(both(z > 0, plane >= z))(lambda: blocks(nx, down_sent.at[plane]).wait_send())
    for plane in range(1, last):
        pl.when(both(z < last, plane <= z))(lambda: blocks(nx, up_sent.at[plane]).wait_send())
    below = both(usual, z < last)
    pl.when(both(below, core == 0))(lambda: blocks(nx - 1, up_sent.at[0]).wait_send())
    pl.when(both(below, core == 1))(lambda: blocks(nx, up_sent.at[0]).wait_send())
    pl.when(both(below, core == 1))(lambda: blocks(1, first_up_sent).wait_send())
    pl.when(both(usual, core == 1))(lambda: blocks(1, first_pair_sent).wait_send())
    pl.when(both(usual, core == 0))(lambda: blocks(1, first_pair_sem).wait_recv())
    handed = chips * CORES * nx - 1 - CORES * nx
    pl.when(helper)(lambda: blocks(1, direct_sent).wait_send())
    pl.when(relays)(lambda: remote(relayed, relayed, relay_sent, relay_sent, pair).wait_send())

    @pl.when(stand_in)
    def _():
        blocks(2 * nx - 1, up_sent.at[0]).wait_send()
        blocks(handed, bulk_sent).wait_send()

    @pl.when(first)
    def _():
        blocks(nx + 1, first_sent).wait_send()
        blocks(handed, bulk_sem).wait_recv()
        for of_core in range(CORES):
            for of_x in range(nx):
                direct(of_core, of_x).wait_recv()


def attend(length, queries, cache, fresh):
    layers, head = queries.shape
    scale = 1.0 / math.sqrt(head)
    every = range(layers)
    keys = [cache[0, layer].reshape(CTX, head) for layer in every]
    values = [cache[1, layer].reshape(CTX, head) for layer in every]
    q = [jnp.broadcast_to(queries[layer : layer + 1], (8, head)) for layer in every]
    contract = (((1,), (1,)), ((), ()))
    scores = [lax.dot_general(q[i], keys[i], contract, preferred_element_type=jnp.float32) * scale for i in every]
    new = [jnp.sum(q[i].astype(jnp.float32) * fresh(0, i), axis=1, keepdims=True) * scale for i in every]
    visible = lax.broadcasted_iota(jnp.int32, scores[0].shape, 1) < length
    scores = [jnp.where(visible, s, -1e30) for s in scores]
    top = [jnp.maximum(jnp.max(s, axis=1, keepdims=True), n) for s, n in zip(scores, new)]
    weights = [jnp.where(visible, jnp.exp(s - t), 0.0) for s, t in zip(scores, top)]
    new = [jnp.exp(n - t) for n, t in zip(new, top)]
    total = [jnp.sum(w, axis=1, keepdims=True) + n for w, n in zip(weights, new)]
    mixed = [jnp.dot(weights[i].astype(values[i].dtype), values[i], preferred_element_type=jnp.float32) for i in every]
    return [(mixed[i] + new[i] * fresh(1, i)) / total[i] for i in every]


def page_kernel(lengths, slots, cache, queries, new_kv, pool, out, tile, sem, tile_sem):
    kinds, layers, pages, head = cache.shape[0], cache.shape[1], cache.shape[2], cache.shape[4]
    length = lengths[0]
    page_now, row_now = length // PAGE, lax.rem(length, PAGE)
    head_now = lax.axis_index("tp") * KVH // lax.axis_size("tp")
    rows = lax.broadcasted_iota(jnp.int32, (PAGE, head), 0)

    def place(page):
        return pool.at[:, :, 0, slots[0, page]]

    def put(step, _):
        page = lax.rem(page_now + step, pages)
        pltpu.make_async_copy(cache.at[:, :, page], place(page), sem).start()
        return 0

    looped = 135
    lax.fori_loop(1, looped + 1, put, 0, unroll=15)
    for step in range(looped + 1, pages):
        put(step, 0)

    def fresh(kind, layer):
        block = new_kv[kind, layer, 0].astype(jnp.float32)
        mine = lax.broadcasted_iota(jnp.int32, block.shape, 0) == head_now
        return jnp.sum(jnp.where(mine, block, 0.0), axis=0, keepdims=True)

    for kind in range(kinds):
        for layer in range(layers):
            held = cache[kind, layer, page_now].astype(jnp.float32)
            tile[kind, layer] = jnp.where(rows == row_now, fresh(kind, layer), held).astype(tile.dtype)
    placed = pltpu.make_async_copy(tile, place(page_now), tile_sem)
    placed.start()
    for layer, mixed in enumerate(attend(length, queries, cache, fresh)):
        out[layer : layer + 1] = mixed[:1].astype(out.dtype)
    others = pl.ds(1, pages - 1)
    pltpu.make_async_copy(cache.at[:, :, others], pool.at[:, :, 0, others], sem).wait()
    placed.wait()


def body(kv_prefill, queries, new_kv, lengths, page_slots):
    kinds, layers, seqs, positions, head = kv_prefill.shape
    nx = lax.axis_size("seq")
    fan = lax.axis_size("tp") // KVH
    chips = fan // CORES
    pages = CTX // PAGE
    pieces = kinds * layers
    dma = pltpu.SemaphoreType.DMA
    anywhere = pl.BlockSpec(memory_space=pl.ANY)
    vmem = pl.BlockSpec(memory_space=pltpu.VMEM)
    smem = pl.BlockSpec(memory_space=pltpu.SMEM)
    cache_shape = (kinds, layers, pages, PAGE, head)
    blocks = kv_prefill.reshape(kinds, layers, seqs, positions // PAGE, PAGE, head)
    hbm = pl.BlockSpec(memory_space=pltpu.HBM)
    small = (page_slots, queries.reshape(layers, head), new_kv)
    cache, *small = pl.pallas_call(
        spread_kernel,
        out_shape=(
            pltpu.VMEM(cache_shape, kv_prefill.dtype),
            pltpu.SMEM(page_slots.shape, page_slots.dtype),
            pltpu.VMEM((layers, head), queries.dtype),
            pltpu.VMEM(new_kv.shape, new_kv.dtype),
        ),
        in_specs=[hbm] * 4,
        out_specs=(vmem, smem, vmem, vmem),
        scratch_shapes=[
            dma((fan * nx,)),
            dma((chips,)),
            dma((pieces,)),
            dma,
            dma,
            dma((CORES * nx,)),
            dma((pieces // 2,)),
            dma,
            dma((chips,)),
            dma((chips,)),
            dma((chips,)),
            dma,
            dma,
            dma,
            dma,
            dma,
            dma,
            dma,
            dma((3,)),
            pltpu.SemaphoreType.REGULAR,
            pltpu.SemaphoreType.REGULAR,
            pltpu.VMEM((pieces // 2, positions // PAGE, PAGE, head), kv_prefill.dtype),
        ],
        compiler_params=pltpu.CompilerParams(collective_id=0, has_side_effects=True, vmem_limit_bytes=16 * MIB),
        name="spread",
    )(*(pltpu.with_memory_space_constraint(a, pltpu.HBM) for a in (blocks, *small)))
    pool, out = pl.pallas_call(
        page_kernel,
        out_shape=(
            jax.ShapeDtypeStruct((kinds, layers, 1, pages, PAGE, head), kv_prefill.dtype),
            jax.ShapeDtypeStruct((layers, head), queries.dtype),
        ),
        in_specs=[smem, smem, vmem, vmem, vmem],
        out_specs=(anywhere, vmem),
        scratch_shapes=[pltpu.VMEM((kinds, layers, PAGE, head), kv_prefill.dtype), dma, dma],
        compiler_params=pltpu.CompilerParams(vmem_limit_bytes=24 * MIB),
        name="pages",
    )(lengths, small[0], cache, *small[1:])
    return pool, out.reshape(queries.shape)


def solution(mesh):
    placed = (
        P(None, None, "groups", ("tp", "seq"), None),
        P(None, ("groups", "seq"), "tp", None),
        P(None, None, ("groups", "seq"), None, None),
        P(("groups", "seq")),
        P(("groups", "seq"), None),
    )
    return jax.shard_map(
        body,
        mesh=mesh,
        in_specs=placed,
        out_specs=(
            P(None, None, "tp", ("groups", "seq"), None, None),
            P(None, ("groups", "seq"), "tp", None),
        ),
        check_vma=False,
    )
```
